32 devices in a mesh: rep: 1 (over z), dp: 32 (over x, y, core).
Axes of the slice: x: 4, y: 4, z: 1, core: 2. Of those that a mesh axis runs over, the one named last changes fastest.
The devices are a block of a 4x4x8 slice.
Arguments:
- x: bfloat16 [32, 2048, 512], P(('rep', 'dp'))
- dy: bfloat16 [32, 2048, 512], P(('rep', 'dp'))
- wq: bfloat16 [2, 512, 512], P(None, 'dp')
- wk: bfloat16 [2, 512, 512], P(None, 'dp')
- wv: bfloat16 [2, 512, 512], P(None, 'dp')
- wo: bfloat16 [2, 512, 512], P(None, 'dp')
- w_gate: bfloat16 [2, 512, 2048], P(None, 'dp')
- w_up: bfloat16 [2, 512, 2048], P(None, 'dp')
- w_down: bfloat16 [2, 2048, 512], P(None, 'dp')
- m_wq: float32 [2, 512, 512], P(None, 'dp')
- m_wk: float32 [2, 512, 512], P(None, 'dp')
- m_wv: float32 [2, 512, 512], P(None, 'dp')
- m_wo: float32 [2, 512, 512], P(None, 'dp')
- m_w_gate: float32 [2, 512, 2048], P(None, 'dp')
- m_w_up: float32 [2, 512, 2048], P(None, 'dp')
- m_w_down: float32 [2, 2048, 512], P(None, 'dp')
- v_wq: float32 [2, 512, 512], P(None, 'dp')
- v_wk: float32 [2, 512, 512], P(None, 'dp')
- v_wv: float32 [2, 512, 512], P(None, 'dp')
- v_wo: float32 [2, 512, 512], P(None, 'dp')
- v_w_gate: float32 [2, 512, 2048], P(None, 'dp')
- v_w_up: float32 [2, 512, 2048], P(None, 'dp')
- v_w_down: float32 [2, 2048, 512], P(None, 'dp')
Outputs:
- output 1: bfloat16 [2, 512, 512], P('rep', 'dp')
- output 2: bfloat16 [2, 512, 512], P('rep', 'dp')
- output 3: bfloat16 [2, 512, 512], P('rep', 'dp')
- output 4: bfloat16 [2, 512, 512], P('rep', 'dp')
- output 5: bfloat16 [2, 512, 2048], P('rep', 'dp')
- output 6: bfloat16 [2, 512, 2048], P('rep', 'dp')
- output 7: bfloat16 [2, 2048, 512], P('rep', 'dp')
- output 8: float32 [2, 512, 512], P('rep', 'dp')
- output 9: float32 [2, 512, 512], P('rep', 'dp')
- output 10: float32 [2, 512, 512], P('rep', 'dp')
- output 11: float32 [2, 512, 512], P('rep', 'dp')
- output 12: float32 [2, 512, 2048], P('rep', 'dp')
- output 13: float32 [2, 512, 2048], P('rep', 'dp')
- output 14: float32 [2, 2048, 512], P('rep', 'dp')
- output 15: float32 [2, 512, 512], P('rep', 'dp')
- output 16: float32 [2, 512, 512], P('rep', 'dp')
- output 17: float32 [2, 512, 512], P('rep', 'dp')
- output 18: float32 [2, 512, 512], P('rep', 'dp')
- output 19: float32 [2, 512, 2048], P('rep', 'dp')
- output 20: float32 [2, 512, 2048], P('rep', 'dp')
- output 21: float32 [2, 2048, 512], P('rep', 'dp')
All inputs are finite; a program needn't handle non-finite values.
Results may differ from the reference program's by a relative error of at most 0.0288.
Values are sent between devices in bfloat16 or wider.
A program may use at most 768 MiB of HBM per device.

```python
import jax
import jax.numpy as jnp
from jax import lax

SEQUENCES = 32
TOKENS = 2048
D = 512
HEADS = 2
KV_HEADS = 2
HEAD = 256
FF = 2048
LAYERS = 2
THETA = 10000
NAMES = ("wq", "wk", "wv", "wo", "w_gate", "w_up", "w_down")
SHAPES = {
    "wq": (LAYERS, D, HEADS * HEAD),
    "wk": (LAYERS, D, KV_HEADS * HEAD),
    "wv": (LAYERS, D, KV_HEADS * HEAD),
    "wo": (LAYERS, HEADS * HEAD, D),
    "w_gate": (LAYERS, D, FF),
    "w_up": (LAYERS, D, FF),
    "w_down": (LAYERS, FF, D),
}


def bump(key, n, height):
    away = (jnp.arange(n, dtype=jnp.int32) - jax.random.randint(key, (), 0, n, jnp.int32)) % n
    return jnp.where(away < n // 8, height, 1.0)


def together(key, own, strength):
    shared = jax.random.normal(key, own.shape[1:], jnp.float32)
    return (own + strength * shared) * lax.rsqrt(1 + strength * strength)


def setup_inputs(seed: int = 0, part: int = 0) -> dict:
    kx, kdy, ka, kb, kz, kf, kh, kl, *keys = jax.random.split(jax.random.key(seed), 8 + 3 * len(NAMES))
    kx, kdy, ka, kb = (jax.random.fold_in(k, part) for k in (kx, kdy, ka, kb))
    kw, km, kv = (keys[i::3] for i in range(3))
    shape = (SEQUENCES, TOKENS, D)
    much_x, much_dy = jax.random.uniform(kz, (2,), jnp.float32, 0.0, 1.0)
    loud = 2.0 ** jax.random.uniform(jax.random.fold_in(kz, 1), (), jnp.float32, -1.0, 2.0)
    layers = 2.0 ** jax.random.uniform(kl, (LAYERS, 1, 1), jnp.float32, -1.0, 1.0)
    times = {"wq": 1.0, "wk": 1.0, "wv": 2.0, "wo": layers, "w_gate": 1.0, "w_up": bump(kh, FF, 4.0), "w_down": layers}
    x = together(ka, jax.random.normal(kx, shape, jnp.float32), much_x) * bump(kf, D, 4.0)
    dy = together(kb, jax.random.normal(kdy, shape, jnp.float32), much_dy)
    drawn = {"x": x.astype(jnp.bfloat16), "dy": (loud * dy * (SEQUENCES * TOKENS) ** -0.5).astype(jnp.bfloat16)}
    for key, name in zip(kw, NAMES, strict=True):
        drawn[name] = (jax.random.normal(key, SHAPES[name], jnp.float32) * SHAPES[name][1] ** -0.5 * times[name]).astype(jnp.bfloat16)
    for key, name in zip(km, NAMES, strict=True):
        drawn[f"m_{name}"] = 0.1 * jax.random.normal(key, SHAPES[name], jnp.float32)
    for key, name in zip(kv, NAMES, strict=True):
        drawn[f"v_{name}"] = jax.random.uniform(key, SHAPES[name], jnp.float32, 0.02, 0.06)
    return drawn


def matmul(a, w):
    return jnp.dot(a, w, preferred_element_type=jnp.float32).astype(jnp.bfloat16)


def normed(h):
    wide = h.astype(jnp.float32)
    scale = lax.rsqrt(jnp.mean(wide**2, -1, keepdims=True) + 1e-6)
    return (wide * scale).astype(jnp.bfloat16)


def turned(t, theta):
    half = t.shape[-1] // 2
    angle = jnp.arange(t.shape[0], dtype=jnp.float32)[:, None] * theta ** (-jnp.arange(half, dtype=jnp.float32) / half)
    cos, sin = jnp.cos(angle)[:, None], jnp.sin(angle)[:, None]
    a, b = t[..., :half].astype(jnp.float32), t[..., half:].astype(jnp.float32)
    return jnp.concatenate([a * cos - b * sin, b * cos + a * sin], -1).astype(jnp.bfloat16)


def seen_by(q, k, v):
    tokens, kv = q.shape[0], k.shape[1]
    q = q.reshape(tokens, kv, -1, q.shape[-1])
    scores = jnp.einsum("tgsd,ugd->gstu", q.astype(jnp.float32), k.astype(jnp.float32)) * q.shape[-1] ** -0.5
    place = jnp.arange(tokens)
    weights = jax.nn.softmax(jnp.where(place[:, None] >= place, scores, -jnp.inf), -1).astype(jnp.bfloat16)
    return jnp.einsum("gstu,ugd->tgsd", weights.astype(jnp.float32), v.astype(jnp.float32)).astype(jnp.bfloat16).reshape(tokens, -1)


def layer(h, w):
    a = normed(h)
    q, k = (turned(matmul(a, w[name]).reshape(h.shape[0], -1, HEAD), THETA) for name in ("wq", "wk"))
    h = h + matmul(seen_by(q, k, matmul(a, w["wv"]).reshape(h.shape[0], -1, HEAD)), w["wo"])
    b = normed(h)
    gate = jnp.dot(b, w["w_gate"], preferred_element_type=jnp.float32)
    up = jnp.dot(b, w["w_up"], preferred_element_type=jnp.float32)
    return h + matmul((jax.nn.silu(gate) * up).astype(jnp.bfloat16), w["w_down"])


def adamw(w, m, v, g):
    m = 0.9 * m + 0.1 * g
    v = 0.95 * v + 0.05 * g * g
    step = m * lax.rsqrt(v + 1e-8) + 0.1 * w
    return (w - 0.02 * step).astype(jnp.bfloat16), m, v


def clipped(gradients, sum_of_squares, count):
    factor = jnp.minimum(1.0, 0.5 * lax.rsqrt(sum_of_squares / count + 1e-30))
    return [g * factor for g in gradients]


def stack(weights, h):
    return lax.scan(lambda h, w: (layer(h, w), None), h, weights)[0]


def reference(x, dy, wq, wk, wv, wo, w_gate, w_up, w_down, m_wq, m_wk, m_wv, m_wo, m_w_gate, m_w_up, m_w_down, v_wq, v_wk, v_wv, v_wo, v_w_gate, v_w_up, v_w_down):
    weights = dict(zip(NAMES, (wq, wk, wv, wo, w_gate, w_up, w_down), strict=True))

    def take(so_far, sequence):
        h, by_y = sequence
        _, back = jax.vjp(stack, weights, h)
        by_weights, by_h = back(by_y)
        return jax.tree.map(lambda total, term: total + term.astype(jnp.float32), so_far, by_weights), by_h

    none_yet = {name: jnp.zeros(w.shape, jnp.float32) for name, w in weights.items()}
    by_weights, by_x = lax.scan(take, none_yet, (x, dy))
    gradients = [by_weights[name].astype(jnp.bfloat16).astype(jnp.float32) for name in NAMES]
    gradients = clipped(gradients, sum(jnp.sum(g * g) for g in gradients), sum(g.size for g in gradients))
    first = (m_wq, m_wk, m_wv, m_wo, m_w_gate, m_w_up, m_w_down)
    second = (v_wq, v_wk, v_wv, v_wo, v_w_gate, v_w_up, v_w_down)
    new = [adamw(weights[name].astype(jnp.float32), m, v, g) for name, m, v, g in zip(NAMES, first, second, gradients, strict=True)]
    return tuple(one[which] for which in range(3) for one in new)
```

```python
import functools
import math

import jax
import jax.numpy as jnp
from jax import lax
from jax.experimental import pallas as pl
from jax.experimental.pallas import tpu as pltpu
from jax.sharding import PartitionSpec as P

HEAD = 256
THETA = 10000
NEG = -1e30
LOG2E = math.log2(math.e)
VMEM = 60 * 2**20
QUERIES = 512
TILE = 512
CHUNK = 512
EPS = 1e-6
BOTH = (0, 1)
STEP = (1, -1)
WAYS = tuple(enumerate(STEP))
bf16, f32 = jnp.bfloat16, jnp.float32


def _dot(a, b, ca=1, cb=0):
    return lax.dot_general(a, b, (((ca,), (cb,)), ((), ())), preferred_element_type=f32)


def _params(semantics, limit=VMEM):
    return pltpu.CompilerParams(dimension_semantics=semantics, vmem_limit_bytes=limit)


def _cost(flops, *arrays):
    return pl.CostEstimate(flops=flops, transcendentals=0, bytes_accessed=sum(a.size * a.dtype.itemsize for a in arrays))


def _attend(q_ref, k_ref, v_ref, o_ref, lse_ref, top_s, mix_s, *, scale):
    heads, size, d = q_ref.shape
    iq = pl.program_id(0)
    e = scale * LOG2E
    top_s[...] = jnp.full(top_s.shape, NEG, f32)
    mix_s[...] = jnp.zeros(mix_s.shape, f32)
    ones = jnp.ones((mix_s.shape[1] - d, size), bf16)

    def block(j, masked):
        here = pl.ds(j * size, size)
        scores = [_dot(k_ref[i, here, :], q_ref[i], 1, 1) for i in range(heads)]
        if masked:
            ok = lax.broadcasted_iota(jnp.int32, (size, size), 1) >= lax.broadcasted_iota(jnp.int32, (size, size), 0)
        weights, keeps = [], []
        for i, s in enumerate(scores):
            if masked:
                s = jnp.where(ok, s, 2 * NEG)
            old = top_s[i : i + 1, :]
            top = jnp.maximum(old, s.max(axis=0, keepdims=True))
            top_s[i : i + 1, :] = top
            weights.append(jnp.exp2((s - top) * e).astype(bf16))
            keeps.append(jnp.exp2((old - top) * e))
        for i in range(heads):
            values = jnp.concatenate([v_ref[i, here, :].T, ones], axis=0)
            mix_s[i] = mix_s[i] * keeps[i] + _dot(values, weights[i])

    lax.fori_loop(0, iq, lambda j, _: block(j, False), None)
    block(iq, True)
    for i in range(heads):
        total = mix_s[i, d : d + 1, :]
        o_ref[i] = (mix_s[i, :d, :] * (1 / total)).T.astype(bf16)
        lse_ref[i : i + 1, :] = top_s[i : i + 1, :] * scale + jnp.log(total)


def attend(q, k, v):
    heads, t, d = q.shape
    size = QUERIES
    block = pl.BlockSpec((heads, size, d), lambda i: (0, i, 0))
    whole = pl.BlockSpec((heads, t, d), lambda i: (0, 0, 0))
    return pl.pallas_call(
        functools.partial(_attend, scale=d**-0.5),
        grid=(t // size,),
        in_specs=[block, whole, whole],
        out_specs=[block, pl.BlockSpec((heads, size), lambda i: (0, i))],
        out_shape=[jax.ShapeDtypeStruct(q.shape, bf16), jax.ShapeDtypeStruct((heads, t), f32)],
        scratch_shapes=[pltpu.VMEM((heads, size), f32), pltpu.VMEM((heads, d + 8, size), f32)],
        compiler_params=_params(("arbitrary",)),
        cost_estimate=_cost(2 * heads * t * t * d, q, k, v, q),
        name="attend",
    )(q, k, v)


def _attend_back(q_ref, k_ref, v_ref, do_ref, lse_ref, delta_ref, dq_ref, dk_ref, dv_ref, dq_s, dk_s, dv_s, *, scale):
    heads, size, d = q_ref.shape
    iq = pl.program_id(0)
    e = scale * LOG2E

    @pl.when(iq == 0)
    def _():
        dk_s[...] = jnp.zeros_like(dk_s)
        dv_s[...] = jnp.zeros_like(dv_s)

    dq_s[...] = jnp.zeros_like(dq_s)
    lses = [lse_ref[i : i + 1, :] * LOG2E for i in range(heads)]

    def block(j, masked):
        here = pl.ds(j * size, size)
        scores = [_dot(k_ref[i, here, :], q_ref[i], 1, 1) for i in range(heads)]
        dps = [_dot(v_ref[i, here, :], do_ref[i], 1, 1) for i in range(heads)]
        if masked:
            ok = lax.broadcasted_iota(jnp.int32, (size, size), 1) >= lax.broadcasted_iota(jnp.int32, (size, size), 0)
        for i in range(heads):
            p = jnp.exp2(scores[i] * e - lses[i])
            if masked:
                p = jnp.where(ok, p, 0.0)
            ds = (p * (dps[i] - delta_ref[i : i + 1, :])).astype(bf16)
            dv_s[i, here, :] += _dot(p.astype(bf16), do_ref[i])
            dk_s[i, here, :] += _dot(ds, q_ref[i])
            dq_s[i] += _dot(k_ref[i, here, :].T, ds)

    lax.fori_loop(0, iq, lambda j, _: block(j, False), None)
    block(iq, True)
    for i in range(heads):
        dq_ref[i] = (dq_s[i] * scale).T.astype(bf16)

    @pl.when(iq == pl.num_programs(0) - 1)
    def _():
        dk_ref[...] = (dk_s[...] * scale).astype(bf16)
        dv_ref[...] = dv_s[...].astype(bf16)


def attend_back(q, k, v, do, lse, delta):
    heads, t, d = q.shape
    size = QUERIES
    block = pl.BlockSpec((heads, size, d), lambda i: (0, i, 0))
    whole = pl.BlockSpec((heads, t, d), lambda i: (0, 0, 0))
    row = pl.BlockSpec((heads, size), lambda i: (0, i))
    return pl.pallas_call(
        functools.partial(_attend_back, scale=d**-0.5),
        grid=(t // size,),
        in_specs=[block, whole, whole, block, row, row],
        out_specs=[block, whole, whole],
        out_shape=[jax.ShapeDtypeStruct(q.shape, bf16)] * 3,
        scratch_shapes=[pltpu.VMEM((heads, d, size), f32), pltpu.VMEM((heads, t, d), f32), pltpu.VMEM((heads, t, d), f32)],
        compiler_params=_params(("arbitrary",)),
        cost_estimate=_cost(5 * heads * t * t * d, q, q, q, q, q, q),
        name="attend_back",
    )(q, k, v, do, lse, delta)


def _scaled(h):
    h = h.astype(f32)
    r = lax.rsqrt(jnp.mean(h * h, -1, keepdims=True) + EPS)
    return h, r, (h * r).astype(bf16)


def _scaled_back(h, r, db):
    return r * db - h * (r * r * r * jnp.mean(db * h, -1, keepdims=True))


def _turned(t, cos, sin):
    half = t.shape[1] // 2
    a, b = t[:, :half].astype(f32), t[:, half:].astype(f32)
    return jnp.concatenate([a * cos - b * sin, b * cos + a * sin], 1).astype(bf16)


def _qkv(h_ref, w_ref, cos_ref, sin_ref, *outs):
    heads, _, d = outs[0].shape
    _, _, a = _scaled(h_ref[...])
    t = _dot(a, w_ref[0]).astype(bf16)
    for n, out in enumerate(outs):
        for i in range(heads):
            at = (n * heads + i) * d
            one = t[:, at : at + d]
            out[i] = one if n == 2 else _turned(one, cos_ref[...], sin_ref[...])


def _qkv_back(h_ref, dq_ref, dk_ref, dv_ref, cos_ref, sin_ref, w_ref, dmid_ref, *rest, inner):
    dh_ref, (dw_ref, acc) = (rest[0], rest[1:]) if inner else (None, rest)
    heads = dq_ref.shape[0]
    step = pl.program_id(0)
    h, r, a = _scaled(h_ref[...])
    back = [_turned(ref[i], cos_ref[...], -sin_ref[...]) for ref in (dq_ref, dk_ref) for i in range(heads)]
    d = jnp.concatenate(back + [dv_ref[i] for i in range(heads)], 1)
    _add_up(step, acc, slice(None), _dot(a.T, d))
    if inner:
        da = _dot(d, w_ref[0], 1, 1).astype(bf16).astype(f32)
        dh_ref[...] = (dmid_ref[...].astype(f32) + _scaled_back(h, r, da)).astype(bf16)

    @pl.when(step == pl.num_programs(0) - 1)
    def _():
        dw_ref[...] = acc[...].astype(bf16)


def _add_up(step, acc, cols, term):
    @pl.when(step == 0)
    def _():
        acc[:, cols] = term

    @pl.when(step > 0)
    def _():
        acc[:, cols] += term


def _middle(h, o_ref, wo_ref):
    d = o_ref.shape[2]
    got = sum(_dot(o_ref[i], wo_ref[0, i * d : (i + 1) * d, :]) for i in range(o_ref.shape[0]))
    return (h.astype(f32) + got.astype(bf16).astype(f32)).astype(bf16)


def _silu(gate):
    s = jax.nn.sigmoid(gate)
    return s, gate * s


def _hidden(h_ref, o_ref, wo_ref, wg_ref, wu_ref, wd_ref, mid_ref, next_ref):
    mid = _middle(h_ref[...], o_ref, wo_ref)
    mid_ref[...] = mid
    h, _, b = _scaled(mid)

    def one(c, total):
        cols = pl.ds(c * CHUNK, CHUNK)
        _, silu = _silu(_dot(b, wg_ref[0, :, cols]))
        act = (silu * _dot(b, wu_ref[0, :, cols])).astype(bf16)
        return total + _dot(act, wd_ref[0, cols, :])

    out = lax.fori_loop(0, wg_ref.shape[2] // CHUNK, one, jnp.zeros(h.shape, f32))
    next_ref[...] = (h + out.astype(bf16).astype(f32)).astype(bf16)


def _hidden_back(h_ref, o_ref, dy_ref, wo_ref, wg_ref, wu_ref, wd_ref, dmid_ref, do_ref, delta_ref, dwo_ref, dwg_ref, dwu_ref, dwd_ref,
                 acc_o, acc_g, acc_u, acc_d, *, last):
    step = pl.program_id(0)
    heads, _, d = o_ref.shape
    h, r, b = _scaled(_middle(h_ref[...], o_ref, wo_ref) if last else h_ref[...])
    dy = dy_ref[...]
    b_t, dy_t = b.T, dy.T

    def one(c, db):
        cols = pl.ds(c * CHUNK, CHUNK)
        s, silu = _silu(_dot(b, wg_ref[0, :, cols]))
        up = _dot(b, wu_ref[0, :, cols])
        dact = _dot(dy, wd_ref[0, cols, :], 1, 1).astype(bf16).astype(f32)
        dup = (dact * silu).astype(bf16)
        dgate = (dact * up * (s + silu - silu * s)).astype(bf16)
        act = (silu * up).astype(bf16)
        _add_up(step, acc_d, cols, _dot(dy_t, act))
        _add_up(step, acc_g, cols, _dot(b_t, dgate))
        _add_up(step, acc_u, cols, _dot(b_t, dup))
        return db + _dot(dgate, wg_ref[0, :, cols], 1, 1) + _dot(dup, wu_ref[0, :, cols], 1, 1)

    db = lax.fori_loop(0, wg_ref.shape[2] // CHUNK, one, jnp.zeros(h.shape, f32)).astype(bf16).astype(f32)
    dmid = (dy.astype(f32) + _scaled_back(h, r, db)).astype(bf16)
    dmid_ref[...] = dmid
    do = _dot(dmid, wo_ref[0], 1, 1).astype(bf16)
    _add_up(step, acc_o, slice(None), _dot(jnp.concatenate([o_ref[i].T for i in range(heads)], 0), dmid))
    for i in range(heads):
        mine = do[:, i * d : (i + 1) * d]
        do_ref[i] = mine
        delta_ref[i : i + 1, :] = jnp.sum((mine.astype(f32) * o_ref[i].astype(f32)).T, axis=0, keepdims=True)

    @pl.when(step == pl.num_programs(0) - 1)
    def _():
        dwo_ref[...] = acc_o[...].astype(bf16)
        dwg_ref[...] = acc_g[...].astype(bf16)
        dwu_ref[...] = acc_u[...].astype(bf16)
        dwd_ref[...] = acc_d[...].T.astype(bf16)


class Layer:
    def __init__(self, number, packed, down, cos, sin):
        self.number, self.packed, self.down, self.cos, self.sin = number, packed, down, cos, sin
        d, f = packed.shape[1], down.shape[1]
        self.d, self.f, self.heads, self.t = d, f, d // HEAD, cos.shape[0]
        once = pl.Buffered(1)
        part = lambda size, at: pl.BlockSpec((1, d, size), lambda i: (number, 0, at // size), pipeline_mode=once)
        self.w_qkv = part(3 * d, 0)
        self.w_hidden = [part(d, 3 * d), part(f, 4 * d), part(f, 4 * d + f), pl.BlockSpec((1, f, d), lambda i: (number, 0, 0), pipeline_mode=once)]
        self.rows = pl.BlockSpec((TILE, d), lambda i: (i, 0))
        self.angle = pl.BlockSpec((TILE, cos.shape[1]), lambda i: (i, 0))
        self.split = pl.BlockSpec((self.heads, TILE, HEAD), lambda i: (0, i, 0))
        self.row = pl.BlockSpec((self.heads, TILE), lambda i: (0, i))
        self.states = jax.ShapeDtypeStruct((self.t, d), bf16)
        self.parts = jax.ShapeDtypeStruct((self.heads, self.t, HEAD), bf16)

    def call(self, body, name, flops, ins, outs, scratch=()):
        arrays = [a for a, _ in ins]
        return pl.pallas_call(
            body, grid=(self.t // TILE,), in_specs=[s for _, s in ins], out_specs=[s for _, s in outs], out_shape=[a for a, _ in outs],
            scratch_shapes=[pltpu.VMEM(s, f32) for s in scratch], compiler_params=_params(("arbitrary",)),
            cost_estimate=_cost(2 * self.t * flops, *arrays), name=name)(*arrays)

    def whole(self, *shape):
        return jax.ShapeDtypeStruct(shape, bf16), pl.BlockSpec(shape, lambda i: (0, 0), pipeline_mode=pl.Buffered(1))

    def hidden_weights(self):
        return [(a, s) for a, s in zip((self.packed,) * 3 + (self.down,), self.w_hidden, strict=True)]

    def qkv(self, h):
        ins = [(h, self.rows), (self.packed, self.w_qkv), (self.cos, self.angle), (self.sin, self.angle)]
        return self.call(_qkv, "qkv", 3 * self.d * self.d, ins, [(self.parts, self.split)] * 3)

    def hidden(self, h, o):
        flops = self.d * self.d + 3 * self.d * self.f
        return self.call(_hidden, "hidden", flops, [(h, self.rows), (o, self.split), *self.hidden_weights()], [(self.states, self.rows)] * 2)

    def hidden_back(self, h, o, dy, last):
        d, f = self.d, self.f
        delta = jax.ShapeDtypeStruct((self.heads, self.t), f32)
        outs = [(self.states, self.rows), (self.parts, self.split), (delta, self.row), self.whole(d, d), self.whole(d, f), self.whole(d, f), self.whole(f, d)]
        return self.call(functools.partial(_hidden_back, last=last), "hidden_back", 3 * d * d + 8 * d * f,
                         [(h, self.rows), (o, self.split), (dy, self.rows), *self.hidden_weights()], outs, [(d, d), (d, f), (d, f), (d, f)])

    def qkv_back(self, h, dqkv, dmid, inner):
        d = self.d
        ins = [(h, self.rows)] + [(a, self.split) for a in dqkv] + [(self.cos, self.angle), (self.sin, self.angle), (self.packed, self.w_qkv), (dmid, self.rows)]
        outs = ([(self.states, self.rows)] if inner else []) + [self.whole(d, 3 * d)]
        return self.call(functools.partial(_qkv_back, inner=inner), "qkv_back", 6 * d * d, ins, outs, [(d, 3 * d)])


def _update(squares_ref, *refs, count):
    (gp_ref, gd_ref), (w, m, v), (new_w, new_m, new_v) = refs[:2], (refs[i : i + 7] for i in (2, 9, 16)), (refs[i : i + 7] for i in (23, 30, 37))
    factor = jnp.minimum(1.0, 0.5 * lax.rsqrt(jnp.sum(squares_ref[...], keepdims=True) / count + 1e-30))
    at = 0
    for i in range(7):
        cols = w[i].shape[2]
        for layer in BOTH:
            g = gd_ref[layer] if i == 6 else gp_ref[layer, :, at : at + cols]
            g = g.astype(f32) * factor
            mm = 0.9 * m[i][layer] + 0.1 * g
            vv = 0.95 * v[i][layer] + 0.05 * g * g
            new_m[i][layer] = mm
            new_v[i][layer] = vv
            old = w[i][layer].astype(f32)
            new_w[i][layer] = (old - 0.02 * (mm * lax.rsqrt(vv + 1e-8) + 0.1 * old)).astype(bf16)
        at += cols


def updated(squares, gp, gd, weights, m, v, count):
    given = [squares, gp, gd, *weights, *m, *v]
    spec = pl.BlockSpec(memory_space=pltpu.VMEM)
    return pl.pallas_call(
        functools.partial(_update, count=count),
        in_specs=[spec] * len(given),
        out_specs=[spec] * 21,
        out_shape=[jax.ShapeDtypeStruct(a.shape, a.dtype) for a in (*weights, *m, *v)],
        compiler_params=pltpu.CompilerParams(vmem_limit_bytes=VMEM),
        cost_estimate=_cost(gp.size, *given),
        name="update",
    )(*given)


MESH = pl.DeviceIdType.MESH


class Place:
    def __init__(self, n):
        self.n, self.side = n, math.isqrt(n // 2)
        self.me = lax.axis_index("dp")
        self.core = lax.rem(self.me, 2)
        chip = lax.div(self.me, 2)
        self.at = (lax.div(chip, self.side), lax.rem(chip, self.side))

    def index(self, x, y, core):
        return (x * self.side + y) * 2 + core

    def moved(self, axis, by):
        at = list(self.at)
        at[axis] = lax.rem(at[axis] + (by + self.side), self.side)
        return self.index(*at, self.core)

    def partner(self):
        return self.index(*self.at, 1 - self.core)

    def off(self, axis, by):
        return lax.rem(self.at[axis] + (by + self.side), self.side)


def _send(src, dst, send, recv, to):
    copy = pltpu.make_async_remote_copy(src_ref=src, dst_ref=dst, send_sem=send, recv_sem=recv, device_id={"dp": to}, device_id_type=MESH)
    copy.start()
    return copy


def _gather(n, p_in, d_in, p_out, d_out, send, recv, pair_send, pair_recv, own_sem):
    me = Place(n)
    partner = me.partner()
    barrier = pltpu.get_barrier_semaphore()
    near = [me.moved(0, 1), me.moved(0, -1), me.moved(1, 1), me.moved(1, -1), partner]
    for to in near:
        pl.semaphore_signal(barrier, inc=1, device_id={"dp": to}, device_id_type=MESH)
    pl.semaphore_wait(barrier, len(near))

    outs = (p_out, d_out)
    wide = p_in.shape[2] // 2
    tall = d_in.shape[1] // 2
    sent = []

    def block(which, layer, i, j, core, half=None):
        x, y = (i, j) if layer == 0 else (j, i)
        ref = outs[which].at[layer, x, y, core]
        if half is None:
            return ref
        return ref.at[:, pl.ds(half * wide, wide)] if which == 0 else ref.at[pl.ds(half * tall, tall), :]

    places = (0, -1, 1, 2)
    order = lambda layer: (layer, 1 - layer)

    def whole(layer, walk, source=None):
        first, second = order(layer)
        i = me.off(first, 0 if walk == 0 else places[walk - 1])
        axis = first if walk == 0 else second
        for d, by in WAYS:
            for which in BOTH:
                dst = block(which, layer, i, me.at[second], me.core)
                sent.append(_send(dst if source is None else source[which].at[layer], dst, send.at[layer, walk, d, which], recv.at[layer, walk, d, which],
                                  me.moved(axis, by)))

    def there(layer, walk, by):
        first, second = order(layer)
        if walk == 0:
            return me.off(first, by), me.at[second]
        return me.off(first, places[walk - 1]), me.off(second, by)

    def forward(layer, walk):
        first, second = order(layer)
        axis = first if walk == 0 else second
        for d, by in WAYS:
            i, j = there(layer, walk, -by)
            for which in BOTH:
                got = block(which, layer, i, j, me.core)
                pltpu.make_async_remote_copy(src_ref=got, dst_ref=got, send_sem=send.at[layer, walk, d, which], recv_sem=recv.at[layer, walk, d, which],
                                             device_id={"dp": me.moved(axis, -by)}, device_id_type=MESH).wait_recv()
                part = block(which, layer, i, j, me.core, d)
                sent.append(_send(part, part, send.at[layer, walk, 2 + d, which], recv.at[layer, walk, 2 + d, which], me.moved(axis, by)))
            share(layer, i, j)

    def finish(layer, walk):
        first, second = order(layer)
        axis = first if walk == 0 else second
        i, j = there(layer, walk, 2)
        for d, by in WAYS:
            for which in BOTH:
                part = block(which, layer, i, j, me.core, d)
                pltpu.make_async_remote_copy(src_ref=part, dst_ref=part, send_sem=send.at[layer, walk, 2 + d, which], recv_sem=recv.at[layer, walk, 2 + d, which],
                                             device_id={"dp": me.moved(axis, -by)}, device_id_type=MESH).wait_recv()
        share(layer, i, j)

    count = [0, 0]
    shared = [[], []]

    def share(layer, i, j, source=None):
        for which in BOTH:
            dst = block(which, layer, i, j, me.core)
            k = count[layer]
            sent.append(_send(dst if source is None else source[which].at[layer], dst, pair_send.at[layer, k, which], pair_recv.at[layer, k, which], partner))
        shared[layer].append((i, j))
        count[layer] += 1

    given = (p_in, d_in)
    own = []
    for layer in BOTH:
        whole(layer, 0, given)
    for layer in BOTH:
        whole(layer, 1, given)
    for layer in BOTH:
        first, second = order(layer)
        share(layer, me.at[first], me.at[second], given)
        for which in BOTH:
            copy = pltpu.make_async_copy(given[which].at[layer], block(which, layer, me.at[first], me.at[second], me.core), own_sem.at[layer, which])
            copy.start()
            own.append(copy)
    for layer in BOTH:
        forward(layer, 0)
        whole(layer, 2)
        whole(layer, 3)
    for layer in BOTH:
        forward(layer, 1)
    for layer in BOTH:
        finish(layer, 0)
        whole(layer, 4)
    for walk in (2, 3):
        for layer in BOTH:
            forward(layer, walk)
    for layer in BOTH:
        finish(layer, 1)
    for layer in BOTH:
        forward(layer, 4)
    for walk in (2, 3, 4):
        for layer in BOTH:
            finish(layer, walk)
    for copy in own:
        copy.wait()
    for layer in BOTH:
        for k, (i, j) in enumerate(shared[layer]):
            for which in BOTH:
                got = block(which, layer, i, j, 1 - me.core)
                pltpu.make_async_remote_copy(src_ref=got, dst_ref=got, send_sem=pair_send.at[layer, k, which], recv_sem=pair_recv.at[layer, k, which],
                                             device_id={"dp": partner}, device_id_type=MESH).wait_recv()
    for copy in sent:
        copy.wait_send()


def gathered(n, weights):
    packed = jnp.concatenate(weights[:6], axis=2)
    down = weights[6]
    side = math.isqrt(n // 2)
    layers, r, wide = packed.shape
    rd, cd = down.shape[1:]
    dma = pltpu.SemaphoreType.DMA
    p, d = pl.pallas_call(
        functools.partial(_gather, n),
        out_shape=[jax.ShapeDtypeStruct((layers, side, side, 2, r, wide), packed.dtype), jax.ShapeDtypeStruct((layers, side, side, 2, rd, cd), down.dtype)],
        in_specs=[pl.BlockSpec(memory_space=pltpu.VMEM)] * 2,
        out_specs=[pl.BlockSpec(memory_space=pl.ANY)] * 2,
        scratch_shapes=[dma((layers, 5, 4, 2)), dma((layers, 5, 4, 2)), dma((layers, side * side, 2)), dma((layers, side * side, 2)), dma((layers, 2))],
        compiler_params=pltpu.CompilerParams(collective_id=1, has_side_effects=True),
        name="gather",
    )(packed, down)
    return p.reshape(layers, n * r, wide), d.reshape(layers, n * rd, cd)


def _reduce(n, *refs):
    grads, rest = (refs[:5], refs[5:10]), refs[10:]
    p_out, d_out, sq_out = rest[:3]
    (own_p, own_d, two_p, two_d, far_p, far_d, near_p, near_d, bfar_p, bfar_d, bnear_p, bnear_d, sq,
     load, pair_send, pair_recv, a_send, a_recv, b_send, b_recv, sq_send, sq_recv) = rest[3:]
    me = Place(n)
    partner, core, side = me.partner(), me.core, me.side
    barrier = pltpu.get_barrier_semaphore()

    def greet(k, _):
        pl.semaphore_signal(barrier, inc=1, device_id={"dp": lax.rem(me.me + k, n)}, device_id_type=MESH)

    lax.fori_loop(1, n, greet, None)
    pl.semaphore_wait(barrier, n - 1)

    own, two = (own_p, own_d), (two_p, two_d)
    order = lambda layer: (layer, 1 - layer)
    places = (2, 1, -1, 0)
    sent = []

    def chunk(layer, k):
        return me.off(order(layer)[0], places[k])

    for k in range(side):
        for layer in BOTH:
            i = chunk(layer, k)
            at = 0
            for w in range(5):
                g = grads[layer][w]
                mine, theirs = ((g.at[i, :, c] if layer == 0 else g.at[:, i, c]) for c in (core, 1 - core))
                which = 0 if w < 4 else 1
                cols = g.shape[4]
                window = lambda buf: buf.at[layer, i, :, :, pl.ds(at, cols)] if which == 0 else buf.at[layer, i]
                pltpu.make_async_copy(mine, window(own[which]), load.at[layer, k, which]).start()
                sent.append(_send(theirs, window(two[which]), pair_send.at[layer, k, which, w], pair_recv.at[layer, k, which], partner))
                at += cols

    def have(layer, k):
        i = chunk(layer, k)
        for which in BOTH:
            pltpu.make_async_copy(own[which].at[layer, i], own[which].at[layer, i], load.at[layer, k, which]).wait()
            got = two[which].at[layer, i]
            pltpu.make_async_remote_copy(src_ref=got, dst_ref=got, send_sem=pair_send.at[layer, k, which, 0], recv_sem=pair_recv.at[layer, k, which],
                                         device_id={"dp": partner}, device_id_type=MESH).wait_recv()

    def both(layer, i, lo, hi):
        def one(j, _):
            for which in BOTH:
                own[which][layer, i, j] = (own[which][layer, i, j].astype(f32) + two[which][layer, i, j].astype(f32)).astype(bf16)
        lax.fori_loop(lo, hi, one, None)

    h = side // 2

    def a_part(which, layer, i, half):
        return own[which].at[layer, i, pl.ds(half * h, h)]

    def a_send_one(layer, d, stage, src, dst):
        by = STEP[d]
        for which in BOTH:
            sent.append(_send(src[which], dst[which], a_send.at[layer, d, stage, which], a_recv.at[layer, d, stage, which], me.moved(order(layer)[0], by)))

    def a_wait(layer, d, stage, dst):
        by = STEP[d]
        for which in BOTH:
            pltpu.make_async_remote_copy(src_ref=dst[which], dst_ref=dst[which], send_sem=a_send.at[layer, d, stage, which], recv_sem=a_recv.at[layer, d, stage, which],
                                         device_id={"dp": me.moved(order(layer)[0], -by)}, device_id_type=MESH).wait_recv()

    far, near = (far_p, far_d), (near_p, near_d)
    far_at = lambda layer, d: [ref.at[layer, d] for ref in far]
    near_at = lambda layer, d, half: [ref.at[layer, d, pl.ds(half * h, h)] for ref in near]
    for layer in BOTH:
        have(layer, 0)
        i = chunk(layer, 0)
        both(layer, i, 0, side)
        for d in BOTH:
            a_send_one(layer, d, 0, [a_part(w, layer, i, d) for w in BOTH], far_at(layer, d))
    for layer in BOTH:
        for d in BOTH:
            have(layer, 1 + d)
            i = chunk(layer, 1 + d)
            both(layer, i, (1 - d) * h, (1 - d) * h + h)
            a_send_one(layer, d, 1, [a_part(w, layer, i, 1 - d) for w in BOTH], near_at(layer, d, 1 - d))
    for layer in BOTH:
        for d in BOTH:
            i = chunk(layer, 1 + d)
            a_wait(layer, d, 0, far_at(layer, d))

            def one(j, _):
                for which in BOTH:
                    b = d * h + j
                    own[which][layer, i, b] = (own[which][layer, i, b].astype(f32) + two[which][layer, i, b].astype(f32)
                                               + far[which][layer, d, j].astype(f32)).astype(bf16)

            lax.fori_loop(0, h, one, None)
            a_send_one(layer, d, 2, [a_part(w, layer, i, d) for w in BOTH], near_at(layer, d, d))
    bfar, bnear = (bfar_p, bfar_d), (bnear_p, bnear_d)
    wide, tall = own_p.shape[4] // 2, own_d.shape[3] // 2

    def half_of(which, ref, half):
        return ref.at[:, pl.ds(half * wide, wide)] if which == 0 else ref.at[pl.ds(half * tall, tall), :]

    def b_send_one(layer, d, stage, src, dst):
        by = STEP[d]
        for which in BOTH:
            sent.append(_send(src[which], dst[which], b_send.at[layer, d, stage, which], b_recv.at[layer, d, stage, which], me.moved(order(layer)[1], by)))

    def b_wait(layer, d, stage, dst):
        by = STEP[d]
        for which in BOTH:
            pltpu.make_async_remote_copy(src_ref=dst[which], dst_ref=dst[which], send_sem=b_send.at[layer, d, stage, which], recv_sem=b_recv.at[layer, d, stage, which],
                                         device_id={"dp": me.moved(order(layer)[1], -by)}, device_id_type=MESH).wait_recv()

    def half_cut(which, half):
        return (slice(None), slice(half * wide, half * wide + wide)) if which == 0 else (slice(half * tall, half * tall + tall), slice(None))

    def four(which, layer, i, j, cut=()):
        return (own[which][(layer, i, j) + cut].astype(f32) + two[which][(layer, i, j) + cut].astype(f32)
                + near[which][(layer, 0, j) + cut].astype(f32) + near[which][(layer, 1, j) + cut].astype(f32))

    bfar_at = lambda layer, d: [ref.at[layer, d] for ref in bfar]
    bnear_at = lambda layer, d, half: [half_of(w, bnear[w].at[layer, d], half) for w in BOTH]
    for layer in BOTH:
        have(layer, 3)
        for d in BOTH:
            a_wait(layer, d, 1, near_at(layer, d, 1 - d))
            a_wait(layer, d, 2, near_at(layer, d, d))
        second = order(layer)[1]
        i = chunk(layer, 3)
        for j, kept in ((me.off(second, 2), None), (me.off(second, 1), 0), (me.off(second, -1), 1)):
            for which in BOTH:
                cut = () if kept is None else half_cut(which, 1 - kept)
                own[which][(layer, i, j) + cut] = four(which, layer, i, j, cut).astype(bf16)
        for d in BOTH:
            j = me.off(second, 2)
            b_send_one(layer, d, 0, [half_of(w, own[w].at[layer, i, j], d) for w in BOTH], bfar_at(layer, d))
        for d in BOTH:
            j = me.off(second, STEP[d])
            b_send_one(layer, d, 1, [half_of(w, own[w].at[layer, i, j], 1 - d) for w in BOTH], bnear_at(layer, d, 1 - d))
    for layer in BOTH:
        second = order(layer)[1]
        i = chunk(layer, 3)
        for d in BOTH:
            j = me.off(second, STEP[d])
            b_wait(layer, d, 0, bfar_at(layer, d))
            for which in BOTH:
                bfar[which][layer, d] = (four(which, layer, i, j, half_cut(which, d)) + bfar[which][layer, d].astype(f32)).astype(bf16)
            b_send_one(layer, d, 2, bfar_at(layer, d), bnear_at(layer, d, d))
    total = jnp.zeros((8, 128), f32)
    for layer in BOTH:
        second = order(layer)[1]
        i, j = chunk(layer, 3), me.at[second]
        for d in BOTH:
            b_wait(layer, d, 1, bnear_at(layer, d, 1 - d))
            b_wait(layer, d, 2, bnear_at(layer, d, d))
        for which, out in ((0, p_out), (1, d_out)):
            g = (four(which, layer, i, j) + bnear[which][layer, 0].astype(f32) + bnear[which][layer, 1].astype(f32)).astype(bf16)
            out[layer] = g
            g = g.astype(f32)
            g = g * g
            rows, cols = g.shape
            total += sum(g[a : a + 8, b : b + 128] for a in range(0, rows, 8) for b in range(0, cols, 128))
    sq[me.me] = total

    def tell(k, _):
        to = lax.rem(me.me + k, n)
        pltpu.make_async_remote_copy(src_ref=sq.at[me.me], dst_ref=sq.at[me.me], send_sem=sq_send.at[k], recv_sem=sq_recv.at[n - k],
                                     device_id={"dp": to}, device_id_type=MESH).start()

    def hear(k, _):
        who = lax.rem(me.me + k, n)
        pltpu.make_async_remote_copy(src_ref=sq.at[who], dst_ref=sq.at[who], send_sem=sq_send.at[k], recv_sem=sq_recv.at[k],
                                     device_id={"dp": who}, device_id_type=MESH).wait_recv()

    def told(k, _):
        to = lax.rem(me.me + k, n)
        pltpu.make_async_remote_copy(src_ref=sq.at[me.me], dst_ref=sq.at[me.me], send_sem=sq_send.at[k], recv_sem=sq_recv.at[n - k],
                                     device_id={"dp": to}, device_id_type=MESH).wait_send()

    lax.fori_loop(1, n, tell, None)
    lax.fori_loop(1, n, hear, None)
    sq_out[...] = jnp.sum(sq[...], axis=0)
    lax.fori_loop(1, n, told, None)
    for copy in sent:
        copy.wait_send()


def reduced(n, grads):
    side = math.isqrt(n // 2)
    layers = len(grads)
    r, rd = grads[0][0].shape[0] // n, grads[0][-1].shape[0] // n
    cd = grads[0][-1].shape[1]
    wide = sum(g.shape[1] for g in grads[0][:-1])
    dma, vmem = pltpu.SemaphoreType.DMA, pltpu.VMEM
    h = side // 2
    cut = [g.reshape(side, side, 2, g.shape[0] // n, g.shape[1]) for layer in grads for g in layer]
    return pl.pallas_call(
        functools.partial(_reduce, n),
        out_shape=[jax.ShapeDtypeStruct((layers, r, wide), bf16), jax.ShapeDtypeStruct((layers, rd, cd), bf16), jax.ShapeDtypeStruct((8, 128), f32)],
        in_specs=[pl.BlockSpec(memory_space=pl.ANY)] * len(cut),
        out_specs=[pl.BlockSpec(memory_space=pltpu.VMEM)] * 3,
        scratch_shapes=[
            vmem((layers, side, side, r, wide), bf16), vmem((layers, side, side, rd, cd), bf16),
            vmem((layers, side, side, r, wide), bf16), vmem((layers, side, side, rd, cd), bf16),
            vmem((layers, 2, h, r, wide), bf16), vmem((layers, 2, h, rd, cd), bf16),
            vmem((layers, 2, side, r, wide), bf16), vmem((layers, 2, side, rd, cd), bf16),
            vmem((layers, 2, r, wide // 2), bf16), vmem((layers, 2, rd // 2, cd), bf16),
            vmem((layers, 2, r, wide), bf16), vmem((layers, 2, rd, cd), bf16),
            vmem((n, 8, 128), f32),
            dma((layers, side, 2)), dma((layers, side, 2, 5)), dma((layers, side, 2)),
            dma((layers, 2, 3, 2)), dma((layers, 2, 3, 2)), dma((layers, 2, 3, 2)), dma((layers, 2, 3, 2)),
            dma((n,)), dma((n,)),
        ],
        compiler_params=pltpu.CompilerParams(collective_id=2, has_side_effects=True, vmem_limit_bytes=48 * 2**20),
        name="reduce",
    )(*cut)


def solution(mesh):
    n = mesh.shape["dp"]

    def step(x, dy, *arrays):
        weights, m, v = (arrays[i : i + 7] for i in (0, 7, 14))
        packed, down = gathered(n, weights)
        half = HEAD // 2
        angle = jnp.arange(x.shape[1], dtype=f32)[:, None] * THETA ** (-jnp.arange(half, dtype=f32) / half)
        first, second = (Layer(i, packed, down, jnp.cos(angle), jnp.sin(angle)) for i in BOTH)
        x = x[0]
        qkv0 = first.qkv(x)
        o0, lse0 = attend(*qkv0)
        mid0, h = first.hidden(x, o0)
        qkv1 = second.qkv(h)
        o1, lse1 = attend(*qkv1)
        dmid, do, delta, *by_hidden1 = second.hidden_back(h, o1, dy[0], True)
        dh, by_qkv1 = second.qkv_back(h, attend_back(*qkv1, do, lse1, delta), dmid, True)
        dmid, do, delta, *by_hidden0 = first.hidden_back(mid0, o0, dh, False)
        (by_qkv0,) = first.qkv_back(x, attend_back(*qkv0, do, lse0, delta), dmid, False)
        gp, gd, squares = reduced(n, [[by_qkv0, *by_hidden0], [by_qkv1, *by_hidden1]])
        return tuple(updated(squares, gp, gd, weights, m, v, n * (gp.size + gd.size)))

    states, cut = P(("rep", "dp"), None, None), P(None, "dp", None)
    return jax.shard_map(
        step,
        mesh=mesh,
        in_specs=(states, states) + (cut,) * 21,
        out_specs=(P("rep", "dp", None),) * 21,
        check_vma=False,
    )
```

```python
import functools
import math

import jax
import jax.numpy as jnp
import numpy as np
from jax import lax
from jax.experimental import pallas as pl
from jax.experimental.pallas import tpu as pltpu
from jax.sharding import PartitionSpec as P

HEAD = 256
THETA = 10000
NEG = -1e30
LOG2E = math.log2(math.e)
VMEM = 60 * 2**20
QUERIES = 512
FINE = 64
TILE = 512
HCHUNK = 512
SUB = 512
CHUNK = 512
EPS = 1e-6
BOTH = (0, 1)
ONCE = pl.Buffered(1)
STEP = (1, -1)
WAYS = tuple(enumerate(STEP))
bf16, f32 = jnp.bfloat16, jnp.float32


def _dot(a, b, ca=1, cb=0):
    return lax.dot_general(a, b, (((ca,), (cb,)), ((), ())), preferred_element_type=f32)


def _dot_t(a, b):
    return _dot(a, b, 1, 1)


def _iota(size, axis):
    return lax.broadcasted_iota(jnp.int32, (size, size), axis)


def _loop(steps, body):
    lax.fori_loop(0, steps, body, None)


PARAMS = pltpu.CompilerParams(dimension_semantics=("arbitrary",), vmem_limit_bytes=VMEM)


def _cost(flops, *arrays):
    return pl.CostEstimate(flops=flops, transcendentals=0, bytes_accessed=sum(a.size * a.dtype.itemsize for a in arrays))


def _strips(iq, count, block):
    def strip(n):
        for j in range(n):
            block(j, False)
        block(n, True)

    for n in range(count):
        pl.when(iq == n)(functools.partial(strip, n))


def _attend(q_ref, k_ref, v_ref, o_ref, lse_ref, top_s, mix_s, *, scale):
    heads, size, d = q_ref.shape
    iq = pl.program_id(0)
    e = scale * LOG2E
    top_s[...] = jnp.full(top_s.shape, NEG, f32)
    mix_s[...] = jnp.zeros(mix_s.shape, f32)
    ones = jnp.ones((mix_s.shape[1] - d, size), bf16)

    def block(j, masked):
        here = pl.ds(j * size, size)
        scores = [_dot_t(k_ref[i, here, :], q_ref[i]) for i in range(heads)]
        if masked:
            ok = _iota(size, 1) >= _iota(size, 0)
        weights, keeps = [], []
        for i, s in enumerate(scores):
            if masked:
                s = jnp.where(ok, s, 2 * NEG)
            old = top_s[i : i + 1, :]
            top = jnp.maximum(old, s.max(axis=0, keepdims=True))
            top_s[i : i + 1, :] = top
            weights.append(jnp.exp2((s - top) * e).astype(bf16))
            keeps.append(jnp.exp2((old - top) * e))
        for i in range(heads):
            values = jnp.concatenate([v_ref[i, here, :].T, ones], axis=0)
            mix_s[i] = mix_s[i] * keeps[i] + _dot(values, weights[i])

    _strips(iq, k_ref.shape[1] // size, block)
    for i in range(heads):
        total = mix_s[i, d : d + 1, :]
        o_ref[i] = (mix_s[i, :d, :] * (1 / total)).T.astype(bf16)
        lse_ref[i : i + 1, :] = top_s[i : i + 1, :] * scale + jnp.log(total)


def attend(q, k, v):
    heads, t, d = q.shape
    size = QUERIES
    block = pl.BlockSpec((heads, size, d), lambda i: (0, i, 0))
    whole = pl.BlockSpec((heads, t, d), lambda i: (0, 0, 0))
    return pl.pallas_call(
        functools.partial(_attend, scale=d**-0.5),
        grid=(t // size,),
        in_specs=[block, whole, whole],
        out_specs=[block, pl.BlockSpec((heads, size), lambda i: (0, i))],
        out_shape=[jax.ShapeDtypeStruct(q.shape, bf16), jax.ShapeDtypeStruct((heads, t), f32)],
        scratch_shapes=[pltpu.VMEM((heads, size), f32), pltpu.VMEM((heads, d + 8, size), f32)],
        compiler_params=PARAMS,
        cost_estimate=_cost(2 * heads * t * t * d, q, k, v, q),
        name="attend",
    )(q, k, v)


def _attend_back(q_ref, k_ref, v_ref, do_ref, lse_ref, delta_ref, dq_ref, dk_ref, dv_ref, dq_s, dk_s, dv_s, *, scale):
    heads, size, d = q_ref.shape
    iq = pl.program_id(0)
    e = scale * LOG2E

    @pl.when(iq == 0)
    def _():
        dk_s[...] = jnp.zeros_like(dk_s)
        dv_s[...] = jnp.zeros_like(dv_s)

    dq_s[...] = jnp.zeros_like(dq_s)
    lses = [lse_ref[i : i + 1, :] * LOG2E for i in range(heads)]

    def block(j, masked):
        here = pl.ds(j * size, size)
        scores = [_dot_t(k_ref[i, here, :], q_ref[i]) for i in range(heads)]
        dps = [_dot_t(v_ref[i, here, :], do_ref[i]) for i in range(heads)]
        ok = _iota(size, 1) >= _iota(size, 0)
        for i in range(heads):
            p = jnp.exp2(scores[i] * e - lses[i])
            if masked:
                p = jnp.where(ok, p, 0.0)
            ds = (p * (dps[i] - delta_ref[i : i + 1, :])).astype(bf16)
            dv_s[i, here, :] += _dot(p.astype(bf16), do_ref[i])
            dk_s[i, here, :] += _dot(ds, q_ref[i])
            dq_s[i] += _dot(k_ref[i, here, :].T, ds)

    _strips(iq, k_ref.shape[1] // size, block)
    for i in range(heads):
        dq_ref[i] = (dq_s[i] * scale).T.astype(bf16)

    @pl.when(iq == pl.num_programs(0) - 1)
    def _():
        dk_ref[...] = (dk_s[...] * scale).astype(bf16)
        dv_ref[...] = dv_s[...].astype(bf16)


def attend_back(q, k, v, do, lse, delta):
    heads, t, d = q.shape
    size = QUERIES
    block = pl.BlockSpec((heads, size, d), lambda i: (0, i, 0))
    whole = pl.BlockSpec((heads, t, d), lambda i: (0, 0, 0))
    row = pl.BlockSpec((heads, size), lambda i: (0, i))
    return pl.pallas_call(
        functools.partial(_attend_back, scale=d**-0.5),
        grid=(t // size,),
        in_specs=[block, whole, whole, block, row, row],
        out_specs=[block, whole, whole],
        out_shape=[jax.ShapeDtypeStruct(q.shape, bf16)] * 3,
        scratch_shapes=[pltpu.VMEM((heads, d, size), f32), pltpu.VMEM((heads, t, d), f32), pltpu.VMEM((heads, t, d), f32)],
        compiler_params=PARAMS,
        cost_estimate=_cost(5 * heads * t * t * d, q, q, q, q, q, q),
        name="attend_back",
    )(q, k, v, do, lse, delta)


def _scaled(h):
    h = h.astype(f32)
    r = lax.rsqrt(jnp.mean(h * h, -1, keepdims=True) + EPS)
    return h, r, (h * r).astype(bf16)


def _scaled_back(h, r, db):
    return r * db - h * (r * r * r * jnp.mean(db * h, -1, keepdims=True))


def _angles(coarse_ref, fine_ref):
    ca, sa = (coarse_ref[i][:, None, :] for i in BOTH)
    cb, sb = (fine_ref[i][None] for i in BOTH)
    shape = (ca.shape[0] * cb.shape[1], ca.shape[2])
    return (ca * cb - sa * sb).reshape(shape), (sa * cb + ca * sb).reshape(shape)


def angle_tables(tokens):
    half = HEAD // 2
    slow = THETA ** (-np.arange(half) / half)
    tables = ((np.arange(0, tokens, FINE), (np.arange(FINE))))
    return [jnp.asarray(np.stack([np.cos(p[:, None] * slow), np.sin(p[:, None] * slow)]), f32) for p in tables]


def _turned(t, cos, sin):
    half = t.shape[1] // 2
    a, b = t[:, :half].astype(f32), t[:, half:].astype(f32)
    return jnp.concatenate([a * cos - b * sin, b * cos + a * sin], 1).astype(bf16)


def _qkv(h_ref, w_ref, coarse_ref, fine_ref, *outs):
    cos, sin = _angles(coarse_ref, fine_ref)
    heads, _, d = outs[0].shape
    _, _, a = _scaled(h_ref[...])
    t = _dot(a, w_ref[...]).astype(bf16)
    for n, out in enumerate(outs):
        for i in range(heads):
            at = (n * heads + i) * d
            one = t[:, at : at + d]
            out[i] = one if n == 2 else _turned(one, cos, sin)


def _qkv_back(h_ref, dq_ref, dk_ref, dv_ref, coarse_ref, fine_ref, w_ref, dmid_ref, *rest, inner):
    dh_ref, (dw_ref, acc) = (rest[0], rest[1:]) if inner else (None, rest)
    heads = dq_ref.shape[0]
    step = pl.program_id(0)
    _cleared(acc)
    h, r, a = _scaled(h_ref[...])
    cos, sin = _angles(coarse_ref, fine_ref)
    back = [_turned(ref[i], cos, -sin) for ref in (dq_ref, dk_ref) for i in range(heads)]
    d = jnp.concatenate(back + [dv_ref[i] for i in range(heads)], 1)
    acc[...] += _dot(a.T, d)
    if inner:
        da = _dot_t(d, w_ref[...]).astype(bf16).astype(f32)
        dh_ref[...] = (dmid_ref[...].astype(f32) + _scaled_back(h, r, da)).astype(bf16)

    @pl.when(step == pl.num_programs(0) - 1)
    def _():
        dw_ref[...] = acc[...].astype(bf16)


def _cleared(*sums):
    @pl.when(pl.program_id(0) == 0)
    def _():
        for ref in sums:
            ref[...] = jnp.zeros(ref.shape, f32)


def _middle(h, o_ref, wo_ref):
    d = o_ref.shape[2]
    got = sum(_dot(o_ref[i], wo_ref[i * d : (i + 1) * d, :]) for i in range(o_ref.shape[0]))
    return (h.astype(f32) + got.astype(bf16).astype(f32)).astype(bf16)


def _silu(gate):
    s = jax.nn.sigmoid(gate)
    return s, gate * s


def _hidden(h_ref, o_ref, wo_ref, wg_ref, wu_ref, wd_ref, mid_ref, next_ref):
    mid = _middle(h_ref[...], o_ref, wo_ref)
    mid_ref[...] = mid
    h, _, b = _scaled(mid)

    def one(c, total):
        cols = pl.ds(c * CHUNK, CHUNK)
        _, silu = _silu(_dot(b, wg_ref[:, cols]))
        act = (silu * _dot(b, wu_ref[:, cols])).astype(bf16)
        return total + _dot(act, wd_ref[cols, :])

    out = lax.fori_loop(0, wg_ref.shape[1] // CHUNK, one, jnp.zeros(h.shape, f32), unroll=True)
    next_ref[...] = (h + out.astype(bf16).astype(f32)).astype(bf16)


def _hidden_back(h_ref, o_ref, dy_ref, wo_ref, wg_ref, wu_ref, wd_ref, dmid_ref, do_ref, delta_ref, dwo_ref, dwg_ref, dwu_ref, dwd_ref,
                 mid_s, b_s, bt_s, dyt_s, db_s, act_s, dgate_s, dup_s, *, last):
    step = pl.program_id(0)
    heads, t, d = o_ref.shape
    tiles = t // TILE

    @pl.when(step == 0)
    def _():
        def one(i, _):
            rows = pl.ds(i * TILE, TILE)
            mid = _middle(h_ref[rows, :], o_ref.at[:, rows, :], wo_ref) if last else h_ref[rows, :]
            mid_s[rows, :] = mid
            b = _scaled(mid)[2]
            b_s[rows, :] = b
            bt_s[:, rows] = b.T
            dyt_s[:, rows] = dy_ref[rows, :].T
            db_s[rows, :] = jnp.zeros((TILE, db_s.shape[1]), f32)

        _loop(tiles, one)

    def part(i, _):
        rows = pl.ds(i * SUB, SUB)
        b = b_s[rows, :]
        s, silu = _silu(_dot(b, wg_ref[...]))
        up = _dot(b, wu_ref[...])
        dact = _dot_t(dy_ref[rows, :], wd_ref[...]).astype(bf16).astype(f32)
        dup = (dact * silu).astype(bf16)
        dgate = (dact * up * (s + silu - silu * s)).astype(bf16)
        act_s[rows, :] = (silu * up).astype(bf16)
        dgate_s[rows, :] = dgate
        dup_s[rows, :] = dup
        db_s[rows, :] += _dot_t(dgate, wg_ref[...]) + _dot_t(dup, wu_ref[...])

    for i in range(t // SUB):
        part(i, None)
    dwd_ref[...] = _dot(dyt_s[...], act_s[...]).T.astype(bf16)
    dwg_ref[...] = _dot(bt_s[...], dgate_s[...]).astype(bf16)
    dwu_ref[...] = _dot(bt_s[...], dup_s[...]).astype(bf16)

    @pl.when(step == pl.num_programs(0) - 1)
    def _():
        def one(i, _):
            rows = pl.ds(i * TILE, TILE)
            h, r, _ = _scaled(mid_s[rows, :])
            db = db_s[rows, :].astype(bf16).astype(f32)
            dmid = (dy_ref[rows, :].astype(f32) + _scaled_back(h, r, db)).astype(bf16)
            dmid_ref[rows, :] = dmid
            do = _dot_t(dmid, wo_ref[...]).astype(bf16)
            for n in range(heads):
                mine, o = do[:, n * d : (n + 1) * d], o_ref[n, rows, :]
                do_ref[n, rows, :] = mine
                delta_ref[n : n + 1, rows] = jnp.sum((mine.astype(f32) * o.astype(f32)).T, axis=0, keepdims=True)
                bt_s[n * d : (n + 1) * d, rows] = o.T

        _loop(tiles, one)
        dwo_ref[...] = _dot(bt_s[...], dmid_ref[...]).astype(bf16)


class Layer:
    def __init__(self, packed, down, tokens, tables):
        self.packed, self.down = packed, down
        d, f = down.shape[1], down.shape[0]
        self.d, self.f, self.heads, self.t = d, f, d // HEAD, tokens
        part = lambda size, at: pl.BlockSpec((d, size), lambda i: (0, at // size), pipeline_mode=ONCE)
        self.w_qkv = part(3 * d, 0)
        self.w_hidden = [part(d, 3 * d), part(f, 4 * d), part(f, 4 * d + f), pl.BlockSpec((f, d), lambda i: (0, 0), pipeline_mode=ONCE)]
        self.rows = pl.BlockSpec((TILE, d), lambda i: (i, 0))
        angle = lambda table, rows, at: pl.BlockSpec((2, rows, table.shape[2]), lambda i: (0, at * i, 0))
        self.angles = [(tables[0], angle(tables[0], TILE // FINE, 1)), (tables[1], angle(tables[1], FINE, 0))]
        self.split = pl.BlockSpec((self.heads, TILE, HEAD), lambda i: (0, i, 0))
        self.row = pl.BlockSpec((self.heads, TILE), lambda i: (0, i))
        self.states = jax.ShapeDtypeStruct((self.t, d), bf16)
        self.parts = jax.ShapeDtypeStruct((self.heads, self.t, HEAD), bf16)

    def call(self, body, name, flops, ins, outs, scratch=()):
        arrays = [a for a, _ in ins]
        return pl.pallas_call(
            body, grid=(self.t // TILE,), in_specs=[s for _, s in ins], out_specs=[s for _, s in outs], out_shape=[a for a, _ in outs],
            scratch_shapes=[pltpu.VMEM(s, f32) for s in scratch], compiler_params=PARAMS,
            cost_estimate=_cost(2 * self.t * flops, *arrays), name=name)(*arrays)

    def whole(self, *shape):
        return jax.ShapeDtypeStruct(shape, bf16), pl.BlockSpec(shape, lambda i: (0, 0), pipeline_mode=ONCE)

    def hidden_weights(self):
        return list(zip((self.packed, self.packed, self.packed, self.down), self.w_hidden))

    def qkv(self, h):
        ins = [(h, self.rows), (self.packed, self.w_qkv), *self.angles]
        return self.call(_qkv, "qkv", 3 * self.d * self.d, ins, [(self.parts, self.split)] * 3)

    def hidden(self, h, o):
        flops = self.d * self.d + 3 * self.d * self.f
        return self.call(_hidden, "hidden", flops, [(h, self.rows), (o, self.split), *self.hidden_weights()], [(self.states, self.rows)] * 2)

    def hidden_back(self, h, o, dy, last):
        d, f, t, size = self.d, self.f, self.t, HCHUNK
        full = lambda *shape: pl.BlockSpec(shape, lambda c: (0,) * len(shape), pipeline_mode=ONCE)
        columns = lambda at: pl.BlockSpec((d, size), lambda c: (0, at // size + c))
        ins = [full(t, d), full(*o.shape), full(t, d), self.w_hidden[0], columns(4 * d), columns(4 * d + f), pl.BlockSpec((size, d), lambda c: (c, 0))]
        slim = pl.BlockSpec((d, size), lambda c: (0, c))
        outs = [full(t, d), full(*o.shape), full(self.heads, t), full(d, d), slim, slim, pl.BlockSpec((size, d), lambda c: (c, 0))]
        shape = lambda *s: jax.ShapeDtypeStruct(s, bf16)
        given = [h, o, dy, self.packed, self.packed, self.packed, self.down]
        vmem = lambda *s: pltpu.VMEM(s, bf16)
        return pl.pallas_call(
            functools.partial(_hidden_back, last=last), grid=(f // size,), in_specs=ins, out_specs=outs,
            out_shape=[self.states, self.parts, jax.ShapeDtypeStruct((self.heads, t), f32), shape(d, d), shape(d, f), shape(d, f), shape(f, d)],
            scratch_shapes=[vmem(t, d), vmem(t, d), vmem(d, t), vmem(d, t), pltpu.VMEM((t, d), f32), vmem(t, size), vmem(t, size), vmem(t, size)],
            compiler_params=PARAMS, cost_estimate=_cost(t * d * f * 16, *given), name="hidden_back")(*given)

    def qkv_back(self, h, dqkv, dmid, inner):
        d = self.d
        ins = [(h, self.rows)] + [(a, self.split) for a in dqkv] + [*self.angles, (self.packed, self.w_qkv), (dmid, self.rows)]
        outs = ([(self.states, self.rows)] if inner else []) + [self.whole(d, 3 * d)]
        return self.call(functools.partial(_qkv_back, inner=inner), "qkv_back", 6 * d * d, ins, outs, [(d, 3 * d)])


def _update(squares_ref, *refs, count):
    (gp_ref, gd_ref), (w, m, v), (new_w, new_m, new_v) = refs[:2], (refs[i : i + 7] for i in (2, 9, 16)), (refs[i : i + 7] for i in (23, 30, 37))
    factor = jnp.minimum(1.0, 0.5 * lax.rsqrt(jnp.sum(squares_ref[...], keepdims=True) / count + 1e-30))
    at = 0
    for i in range(7):
        cols = w[i].shape[2]

        def one(layer, _):
            g = gd_ref[layer] if i == 6 else gp_ref[layer, :, at : at + cols]
            g = g.astype(f32) * factor
            mm = 0.9 * m[i][layer] + 0.1 * g
            vv = 0.95 * v[i][layer] + 0.05 * g * g
            new_m[i][layer] = mm
            new_v[i][layer] = vv
            old = w[i][layer].astype(f32)
            new_w[i][layer] = (old - 0.02 * (mm * lax.rsqrt(vv + 1e-8) + 0.1 * old)).astype(bf16)

        _loop(w[i].shape[0], one)
        at += cols


def updated(squares, gp, gd, weights, m, v, count):
    given = [squares, gp, gd, *weights, *m, *v]
    spec = pl.BlockSpec(memory_space=pltpu.VMEM)
    return pl.pallas_call(
        functools.partial(_update, count=count),
        in_specs=[spec] * len(given),
        out_specs=[spec] * 21,
        out_shape=[jax.ShapeDtypeStruct(a.shape, a.dtype) for a in (*weights, *m, *v)],
        compiler_params=pltpu.CompilerParams(vmem_limit_bytes=VMEM),
        cost_estimate=_cost(gp.size, *given),
        name="update",
    )(*given)


MESH = pl.DeviceIdType.MESH


class Place:
    def __init__(self, n):
        self.n, self.side = n, math.isqrt(n // 2)
        self.me = lax.axis_index("dp")
        self.core = lax.rem(self.me, 2)
        chip = lax.div(self.me, 2)
        self.at = (lax.div(chip, self.side), lax.rem(chip, self.side))

    def index(self, x, y, core):
        return (x * self.side + y) * 2 + core

    def moved(self, axis, by):
        at = list(self.at)
        at[axis] = lax.rem(at[axis] + (by + self.side), self.side)
        return self.index(*at, self.core)

    def partner(self):
        return self.index(*self.at, 1 - self.core)

    def off(self, axis, by):
        return lax.rem(self.at[axis] + (by + self.side), self.side)


def _send(src, dst, send, recv, to):
    copy = pltpu.make_async_remote_copy(src_ref=src, dst_ref=dst, send_sem=send, recv_sem=recv, device_id={"dp": to}, device_id_type=MESH)
    copy.start()
    return copy


def _gather(n, p_in, d_in, *rest):
    outs, (send, recv, pair_send, pair_recv, own_sem) = (rest[:2], rest[2:4]), rest[4:]
    me = Place(n)
    partner = me.partner()
    barrier = pltpu.get_barrier_semaphore()
    near = [me.moved(0, 1), me.moved(0, -1), me.moved(1, 1), me.moved(1, -1), partner]
    for to in near:
        pl.semaphore_signal(barrier, inc=1, device_id={"dp": to}, device_id_type=MESH)
    pl.semaphore_wait(barrier, len(near))

    wide = p_in.shape[2] // 2
    tall = d_in.shape[1] // 2
    sent = []

    def block(which, layer, i, j, core, half=None):
        x, y = (i, j) if layer == 0 else (j, i)
        ref = outs[layer][which].at[x, y, core]
        if half is None:
            return ref
        return ref.at[:, pl.ds(half * wide, wide)] if which == 0 else ref.at[pl.ds(half * tall, tall), :]

    places = (0, -1, 1, 2)
    order = lambda layer: (layer, 1 - layer)

    def whole(layer, walk, source=None):
        first, second = order(layer)
        i = me.off(first, 0 if walk == 0 else places[walk - 1])
        axis = first if walk == 0 else second
        for d, by in WAYS:
            for which in BOTH:
                dst = block(which, layer, i, me.at[second], me.core)
                sent.append(_send(dst if source is None else source[which].at[layer], dst, send.at[layer, walk, d, which], recv.at[layer, walk, d, which],
                                  me.moved(axis, by)))

    def there(layer, walk, by):
        first, second = order(layer)
        if walk == 0:
            return me.off(first, by), me.at[second]
        return me.off(first, places[walk - 1]), me.off(second, by)

    def forward(layer, walk):
        first, second = order(layer)
        axis = first if walk == 0 else second
        for d, by in WAYS:
            i, j = there(layer, walk, -by)
            for which in BOTH:
                got = block(which, layer, i, j, me.core)
                pltpu.make_async_remote_copy(src_ref=got, dst_ref=got, send_sem=send.at[layer, walk, d, which], recv_sem=recv.at[layer, walk, d, which],
                                             device_id={"dp": me.moved(axis, -by)}, device_id_type=MESH).wait_recv()
                part = block(which, layer, i, j, me.core, d)
                sent.append(_send(part, part, send.at[layer, walk, 2 + d, which], recv.at[layer, walk, 2 + d, which], me.moved(axis, by)))
            share(layer, i, j)

    def finish(layer, walk):
        first, second = order(layer)
        axis = first if walk == 0 else second
        i, j = there(layer, walk, 2)
        for d, by in WAYS:
            for which in BOTH:
                part = block(which, layer, i, j, me.core, d)
                pltpu.make_async_remote_copy(src_ref=part, dst_ref=part, send_sem=send.at[layer, walk, 2 + d, which], recv_sem=recv.at[layer, walk, 2 + d, which],
                                             device_id={"dp": me.moved(axis, -by)}, device_id_type=MESH).wait_recv()
        share(layer, i, j)

    count = [0, 0]
    shared = [[], []]

    def share(layer, i, j, source=None):
        for which in BOTH:
            dst = block(which, layer, i, j, me.core)
            k = count[layer]
            sent.append(_send(dst if source is None else source[which].at[layer], dst, pair_send.at[layer, k, which], pair_recv.at[layer, k, which], partner))
        shared[layer].append((i, j))
        count[layer] += 1

    given = (p_in, d_in)
    own = []
    for layer in BOTH:
        whole(layer, 0, given)
    for layer in BOTH:
        whole(layer, 1, given)
    for layer in BOTH:
        first, second = order(layer)
        share(layer, me.at[first], me.at[second], given)
        for which in BOTH:
            copy = pltpu.make_async_copy(given[which].at[layer], block(which, layer, me.at[first], me.at[second], me.core), own_sem.at[layer, which])
            copy.start()
            own.append(copy)
    for layer in BOTH:
        forward(layer, 0)
        whole(layer, 2)
        whole(layer, 3)
    for layer in BOTH:
        forward(layer, 1)
    for layer in BOTH:
        finish(layer, 0)
        whole(layer, 4)
    for walk in (2, 3):
        for layer in BOTH:
            forward(layer, walk)
    for layer in BOTH:
        finish(layer, 1)
    for layer in BOTH:
        forward(layer, 4)
    for walk in (2, 3, 4):
        for layer in BOTH:
            finish(layer, walk)
    for copy in own:
        copy.wait()
    for layer in BOTH:
        for k, (i, j) in enumerate(shared[layer]):
            for which in BOTH:
                got = block(which, layer, i, j, 1 - me.core)
                pltpu.make_async_remote_copy(src_ref=got, dst_ref=got, send_sem=pair_send.at[layer, k, which], recv_sem=pair_recv.at[layer, k, which],
                                             device_id={"dp": partner}, device_id_type=MESH).wait_recv()
    for copy in sent:
        copy.wait_send()


def gathered(n, weights):
    packed = jnp.concatenate(weights[:6], axis=2)
    down = weights[6]
    side = math.isqrt(n // 2)
    layers, r, wide = packed.shape
    rd, cd = down.shape[1:]
    dma = pltpu.SemaphoreType.DMA
    whole = pl.pallas_call(
        functools.partial(_gather, n),
        out_shape=[jax.ShapeDtypeStruct((side, side, 2, *s), bf16) for s in ((r, wide), (rd, cd))] * layers,
        in_specs=[pl.BlockSpec(memory_space=pltpu.VMEM)] * 2,
        out_specs=[pl.BlockSpec(memory_space=pl.ANY)] * (2 * layers),
        scratch_shapes=[dma((layers, 5, 4, 2)), dma((layers, 5, 4, 2)), dma((layers, side * side, 2)), dma((layers, side * side, 2)), dma((layers, 2))],
        compiler_params=pltpu.CompilerParams(collective_id=1, has_side_effects=True),
        name="gather",
    )(packed, down)
    return [[a.reshape(-1, a.shape[-1]) for a in whole[at : at + 2]] for at in range(0, 2 * layers, 2)]


def _reduce(n, *refs):
    grads, rest = (refs[:5], refs[5:10]), refs[10:]
    p_out, d_out, sq_out = rest[:3]
    (own_p, own_d, two_p, two_d, far_p, far_d, near_p, near_d, bfar_p, bfar_d, bnear_p, bnear_d, sq,
     load, pair_send, pair_recv, a_send, a_recv, b_send, b_recv, sq_send, sq_recv) = rest[3:]
    me = Place(n)
    partner, core, side = me.partner(), me.core, me.side
    barrier = pltpu.get_barrier_semaphore()

    def greet(k, _):
        pl.semaphore_signal(barrier, inc=1, device_id={"dp": lax.rem(me.me + k, n)}, device_id_type=MESH)

    lax.fori_loop(1, n, greet, None)
    pl.semaphore_wait(barrier, n - 1)

    own, two = (own_p, own_d), (two_p, two_d)
    order = lambda layer: (layer, 1 - layer)
    places = (2, 1, -1, 0)
    sent = []

    def chunk(layer, k):
        return me.off(order(layer)[0], places[k])

    for k in range(side):
        for layer in BOTH:
            i = chunk(layer, k)
            at = 0
            for w in range(5):
                g = grads[layer][w]
                mine, theirs = ((g.at[i, :, c] if layer == 0 else g.at[:, i, c]) for c in (core, 1 - core))
                which = 0 if w < 4 else 1
                cols = g.shape[4]
                window = lambda buf: buf.at[layer, i, :, :, pl.ds(at, cols)] if which == 0 else buf.at[layer, i]
                pltpu.make_async_copy(mine, window(own[which]), load.at[layer, k, which]).start()
                sent.append(_send(theirs, window(two[which]), pair_send.at[layer, k, which, w], pair_recv.at[layer, k, which], partner))
                at += cols

    def have(layer, k):
        i = chunk(layer, k)
        for which in BOTH:
            pltpu.make_async_copy(own[which].at[layer, i], own[which].at[layer, i], load.at[layer, k, which]).wait()
            got = two[which].at[layer, i]
            pltpu.make_async_remote_copy(src_ref=got, dst_ref=got, send_sem=pair_send.at[layer, k, which, 0], recv_sem=pair_recv.at[layer, k, which],
                                         device_id={"dp": partner}, device_id_type=MESH).wait_recv()

    wide, tall = own_p.shape[4] // 2, own_d.shape[3] // 2
    piece = wide // 2

    def over(which, half, body):
        if which == 1:
            part = slice(None) if half is None else slice(half * tall, half * tall + tall)
            body((part, slice(None)), (slice(None), slice(None)))
        else:
            first = 0 if half is None else 2 * half
            columns = lambda k: (slice(None), pl.ds(pl.multiple_of(k * piece, 128), piece))
            _loop(4 if half is None else 2, lambda k, _: body(columns(first + k), columns(k)))

    def both(layer, i, lo, hi):
        def one(j, _):
            for which in BOTH:
                def body(at, _):
                    own[which][(layer, i, j) + at] = (own[which][(layer, i, j) + at].astype(f32) + two[which][(layer, i, j) + at].astype(f32)).astype(bf16)
                over(which, None, body)
        lax.fori_loop(lo, hi, one, None)

    h = side // 2

    def a_part(which, layer, i, half):
        return own[which].at[layer, i, pl.ds(half * h, h)]

    def a_send_one(layer, d, stage, src, dst):
        by = STEP[d]
        for which in BOTH:
            sent.append(_send(src[which], dst[which], a_send.at[layer, d, stage, which], a_recv.at[layer, d, stage, which], me.moved(order(layer)[0], by)))

    def a_wait(layer, d, stage, dst):
        by = STEP[d]
        for which in BOTH:
            pltpu.make_async_remote_copy(src_ref=dst[which], dst_ref=dst[which], send_sem=a_send.at[layer, d, stage, which], recv_sem=a_recv.at[layer, d, stage, which],
                                         device_id={"dp": me.moved(order(layer)[0], -by)}, device_id_type=MESH).wait_recv()

    far, near = (far_p, far_d), (near_p, near_d)
    far_at = lambda layer, d: [ref.at[layer, d] for ref in far]
    near_at = lambda layer, d, half: [ref.at[layer, d, pl.ds(half * h, h)] for ref in near]
    for layer in BOTH:
        have(layer, 0)
        i = chunk(layer, 0)
        both(layer, i, 0, side)
        for d in BOTH:
            a_send_one(layer, d, 0, [a_part(w, layer, i, d) for w in BOTH], far_at(layer, d))
    for layer in BOTH:
        for d in BOTH:
            have(layer, 1 + d)
            i = chunk(layer, 1 + d)
            both(layer, i, (1 - d) * h, (1 - d) * h + h)
            a_send_one(layer, d, 1, [a_part(w, layer, i, 1 - d) for w in BOTH], near_at(layer, d, 1 - d))
    for layer in BOTH:
        for d in BOTH:
            i = chunk(layer, 1 + d)
            a_wait(layer, d, 0, far_at(layer, d))

            def one(j, _):
                b = d * h + j
                for which in BOTH:
                    def body(at, _):
                        own[which][(layer, i, b) + at] = (own[which][(layer, i, b) + at].astype(f32) + two[which][(layer, i, b) + at].astype(f32)
                                                          + far[which][(layer, d, j) + at].astype(f32)).astype(bf16)
                    over(which, None, body)

            _loop(h, one)
            a_send_one(layer, d, 2, [a_part(w, layer, i, d) for w in BOTH], near_at(layer, d, d))
    bfar, bnear = (bfar_p, bfar_d), (bnear_p, bnear_d)
    def half_of(which, ref, half):
        return ref.at[:, pl.ds(half * wide, wide)] if which == 0 else ref.at[pl.ds(half * tall, tall), :]

    def b_send_one(layer, d, stage, src, dst):
        by = STEP[d]
        for which in BOTH:
            sent.append(_send(src[which], dst[which], b_send.at[layer, d, stage, which], b_recv.at[layer, d, stage, which], me.moved(order(layer)[1], by)))

    def b_wait(layer, d, stage, dst):
        by = STEP[d]
        for which in BOTH:
            pltpu.make_async_remote_copy(src_ref=dst[which], dst_ref=dst[which], send_sem=b_send.at[layer, d, stage, which], recv_sem=b_recv.at[layer, d, stage, which],
                                         device_id={"dp": me.moved(order(layer)[1], -by)}, device_id_type=MESH).wait_recv()

    def four(which, layer, i, j, cut):
        return (own[which][(layer, i, j) + cut].astype(f32) + two[which][(layer, i, j) + cut].astype(f32)
                + near[which][(layer, 0, j) + cut].astype(f32) + near[which][(layer, 1, j) + cut].astype(f32))

    bfar_at = lambda layer, d: [ref.at[layer, d] for ref in bfar]
    bnear_at = lambda layer, d, half: [half_of(w, bnear[w].at[layer, d], half) for w in BOTH]
    for layer in BOTH:
        have(layer, 3)
        for d in BOTH:
            a_wait(layer, d, 1, near_at(layer, d, 1 - d))
            a_wait(layer, d, 2, near_at(layer, d, d))
        second = order(layer)[1]
        i = chunk(layer, 3)
        for j, kept in ((me.off(second, 2), None), (me.off(second, 1), 0), (me.off(second, -1), 1)):
            for which in BOTH:
                def body(at, _):
                    own[which][(layer, i, j) + at] = four(which, layer, i, j, at).astype(bf16)
                over(which, None if kept is None else 1 - kept, body)
        for d in BOTH:
            j = me.off(second, 2)
            b_send_one(layer, d, 0, [half_of(w, own[w].at[layer, i, j], d) for w in BOTH], bfar_at(layer, d))
        for d in BOTH:
            j = me.off(second, STEP[d])
            b_send_one(layer, d, 1, [half_of(w, own[w].at[layer, i, j], 1 - d) for w in BOTH], bnear_at(layer, d, 1 - d))
    for layer in BOTH:
        second = order(layer)[1]
        i = chunk(layer, 3)
        for d in BOTH:
            j = me.off(second, STEP[d])
            b_wait(layer, d, 0, bfar_at(layer, d))
            for which in BOTH:
                def body(at, here):
                    bfar[which][(layer, d) + here] = (four(which, layer, i, j, at) + bfar[which][(layer, d) + here].astype(f32)).astype(bf16)
                over(which, d, body)
            b_send_one(layer, d, 2, bfar_at(layer, d), bnear_at(layer, d, d))
    sq[me.me] = jnp.zeros(sq.shape[1:], f32)
    for layer in BOTH:
        second = order(layer)[1]
        i, j = chunk(layer, 3), me.at[second]
        for d in BOTH:
            b_wait(layer, d, 1, bnear_at(layer, d, 1 - d))
            b_wait(layer, d, 2, bnear_at(layer, d, d))
        for which, out in ((0, p_out), (1, d_out)):
            def body(at, _):
                g = (four(which, layer, i, j, at) + bnear[which][(layer, 0) + at].astype(f32) + bnear[which][(layer, 1) + at].astype(f32)).astype(bf16)
                out[(layer,) + at] = g
                g = g.astype(f32)
                g = g * g
                rows, cols = g.shape
                sq[me.me] += sum(g[a : a + 8, b : b + 128] for a in range(0, rows, 8) for b in range(0, cols, 128))
            over(which, None, body)
    def tell(k, _):
        to = lax.rem(me.me + k, n)
        pltpu.make_async_remote_copy(src_ref=sq.at[me.me], dst_ref=sq.at[me.me], send_sem=sq_send.at[k], recv_sem=sq_recv.at[n - k],
                                     device_id={"dp": to}, device_id_type=MESH).start()

    def hear(k, _):
        who = lax.rem(me.me + k, n)
        pltpu.make_async_remote_copy(src_ref=sq.at[who], dst_ref=sq.at[who], send_sem=sq_send.at[k], recv_sem=sq_recv.at[k],
                                     device_id={"dp": who}, device_id_type=MESH).wait_recv()

    def told(k, _):
        to = lax.rem(me.me + k, n)
        pltpu.make_async_remote_copy(src_ref=sq.at[me.me], dst_ref=sq.at[me.me], send_sem=sq_send.at[k], recv_sem=sq_recv.at[n - k],
                                     device_id={"dp": to}, device_id_type=MESH).wait_send()

    lax.fori_loop(1, n, tell, None)
    lax.fori_loop(1, n, hear, None)
    sq_out[...] = jnp.sum(sq[...], axis=0)
    lax.fori_loop(1, n, told, None)
    for copy in sent:
        copy.wait_send()


def reduced(n, grads):
    side = math.isqrt(n // 2)
    layers = len(grads)
    r, rd = grads[0][0].shape[0] // n, grads[0][-1].shape[0] // n
    cd = grads[0][-1].shape[1]
    wide = sum(g.shape[1] for g in grads[0][:-1])
    dma, vmem = pltpu.SemaphoreType.DMA, pltpu.VMEM
    h = side // 2
    cut = [g.reshape(side, side, 2, g.shape[0] // n, g.shape[1]) for layer in grads for g in layer]
    return pl.pallas_call(
        functools.partial(_reduce, n),
        out_shape=[jax.ShapeDtypeStruct((layers, r, wide), bf16), jax.ShapeDtypeStruct((layers, rd, cd), bf16), jax.ShapeDtypeStruct((8, 128), f32)],
        in_specs=[pl.BlockSpec(memory_space=pl.ANY)] * len(cut),
        out_specs=[pl.BlockSpec(memory_space=pltpu.VMEM)] * 3,
        scratch_shapes=[
            vmem((layers, side, side, r, wide), bf16), vmem((layers, side, side, rd, cd), bf16),
            vmem((layers, side, side, r, wide), bf16), vmem((layers, side, side, rd, cd), bf16),
            vmem((layers, 2, h, r, wide), bf16), vmem((layers, 2, h, rd, cd), bf16),
            vmem((layers, 2, side, r, wide), bf16), vmem((layers, 2, side, rd, cd), bf16),
            vmem((layers, 2, r, wide // 2), bf16), vmem((layers, 2, rd // 2, cd), bf16),
            vmem((layers, 2, r, wide), bf16), vmem((layers, 2, rd, cd), bf16),
            vmem((n, 8, 128), f32),
            dma((layers, side, 2)), dma((layers, side, 2, 5)), dma((layers, side, 2)),
            dma((layers, 2, 3, 2)), dma((layers, 2, 3, 2)), dma((layers, 2, 3, 2)), dma((layers, 2, 3, 2)),
            dma((n,)), dma((n,)),
        ],
        compiler_params=pltpu.CompilerParams(collective_id=2, has_side_effects=True, vmem_limit_bytes=48 * 2**20),
        name="reduce",
    )(*cut)


def solution(mesh):
    n = mesh.shape["dp"]

    def step(x, dy, *arrays):
        weights, m, v = (arrays[i : i + 7] for i in (0, 7, 14))
        whole = gathered(n, weights)
        tables = angle_tables(x.shape[1])
        first, second = (Layer(*w, x.shape[1], tables) for w in whole)
        x = x[0]
        qkv0 = first.qkv(x)
        o0, lse0 = attend(*qkv0)
        mid0, h = first.hidden(x, o0)
        qkv1 = second.qkv(h)
        o1, lse1 = attend(*qkv1)
        dmid, do, delta, *by_hidden1 = second.hidden_back(h, o1, dy[0], True)
        dh, by_qkv1 = second.qkv_back(h, attend_back(*qkv1, do, lse1, delta), dmid, True)
        dmid, do, delta, *by_hidden0 = first.hidden_back(mid0, o0, dh, False)
        (by_qkv0,) = first.qkv_back(x, attend_back(*qkv0, do, lse0, delta), dmid, False)
        gp, gd, squares = reduced(n, [[by_qkv0, *by_hidden0], [by_qkv1, *by_hidden1]])
        return tuple(updated(squares, gp, gd, weights, m, v, n * (gp.size + gd.size)))

    states, cut = P(("rep", "dp"), None, None), P(None, "dp", None)
    return jax.shard_map(
        step,
        mesh=mesh,
        in_specs=(states, states) + (cut,) * 21,
        out_specs=(P("rep", "dp", None),) * 21,
        check_vma=False,
    )
```

```python
import functools
import math

import jax
import jax.numpy as jnp
import numpy as np
from jax import lax
from jax.experimental import pallas as pl
from jax.experimental.pallas import tpu as pltpu
from jax.sharding import PartitionSpec as P

HEAD = 256
THETA = 10000
NEG = -1e30
LOG2E = math.log2(math.e)
VMEM = 60 * 2**20
QUERIES = 512
FINE = 64
TILE = 512
HCHUNK = 512
SUB = 1024
CHUNK = 512
EPS = 1e-6
BOTH = (0, 1)
ONCE = pl.Buffered(1)
STEP = (1, -1)
WAYS = tuple(enumerate(STEP))
bf16, f32 = jnp.bfloat16, jnp.float32


def _dot(a, b, ca=1, cb=0):
    return lax.dot_general(a, b, (((ca,), (cb,)), ((), ())), preferred_element_type=f32)


def _dot_t(a, b):
    return _dot(a, b, 1, 1)


def _iota(size, axis):
    return lax.broadcasted_iota(jnp.int32, (size, size), axis)


def _loop(steps, body):
    lax.fori_loop(0, steps, body, None)


PARAMS = pltpu.CompilerParams(dimension_semantics=("arbitrary",), vmem_limit_bytes=VMEM)


def _cost(flops, *arrays):
    return pl.CostEstimate(flops=flops, transcendentals=0, bytes_accessed=sum(a.size * a.dtype.itemsize for a in arrays))


def _strips(iq, count, block):
    def strip(n):
        for j in range(n):
            block(j, False)
        block(n, True)

    for n in range(count):
        pl.when(iq == n)(functools.partial(strip, n))


def _attend(q_ref, k_ref, v_ref, o_ref, lse_ref, top_s, mix_s, *, scale):
    heads, size, d = q_ref.shape
    iq = pl.program_id(0)
    e = scale * LOG2E
    top_s[...] = jnp.full(top_s.shape, NEG, f32)
    mix_s[...] = jnp.zeros(mix_s.shape, f32)
    ones = jnp.ones((mix_s.shape[1] - d, size), bf16)

    def block(j, masked):
        here = pl.ds(j * size, size)
        scores = [_dot_t(k_ref[i, here, :], q_ref[i]) for i in range(heads)]
        if masked:
            ok = _iota(size, 1) >= _iota(size, 0)
        weights, keeps = [], []
        for i, s in enumerate(scores):
            if masked:
                s = jnp.where(ok, s, 2 * NEG)
            old = top_s[i : i + 1, :]
            top = jnp.maximum(old, s.max(axis=0, keepdims=True))
            top_s[i : i + 1, :] = top
            weights.append(jnp.exp2((s - top) * e).astype(bf16))
            keeps.append(jnp.exp2((old - top) * e))
        for i in range(heads):
            values = jnp.concatenate([v_ref[i, here, :].T, ones], axis=0)
            mix_s[i] = mix_s[i] * keeps[i] + _dot(values, weights[i])

    _strips(iq, k_ref.shape[1] // size, block)
    for i in range(heads):
        total = mix_s[i, d : d + 1, :]
        o_ref[i] = (mix_s[i, :d, :] * (1 / total)).T.astype(bf16)
        lse_ref[i : i + 1, :] = top_s[i : i + 1, :] * scale + jnp.log(total)


def attend(q, k, v):
    heads, t, d = q.shape
    size = QUERIES
    block = pl.BlockSpec((heads, size, d), lambda i: (0, i, 0))
    whole = pl.BlockSpec((heads, t, d), lambda i: (0, 0, 0))
    return pl.pallas_call(
        functools.partial(_attend, scale=d**-0.5),
        grid=(t // size,),
        in_specs=[block, whole, whole],
        out_specs=[block, pl.BlockSpec((heads, size), lambda i: (0, i))],
        out_shape=[jax.ShapeDtypeStruct(q.shape, bf16), jax.ShapeDtypeStruct((heads, t), f32)],
        scratch_shapes=[pltpu.VMEM((heads, size), f32), pltpu.VMEM((heads, d + 8, size), f32)],
        compiler_params=PARAMS,
        cost_estimate=_cost(2 * heads * t * t * d, q, k, v, q),
        name="attend",
    )(q, k, v)


def _attend_back(q_ref, k_ref, v_ref, do_ref, lse_ref, delta_ref, dq_ref, dk_ref, dv_ref, dq_s, dk_s, dv_s, *, scale):
    heads, size, d = q_ref.shape
    iq = pl.program_id(0)
    e = scale * LOG2E

    @pl.when(iq == 0)
    def _():
        dk_s[...] = jnp.zeros_like(dk_s)
        dv_s[...] = jnp.zeros_like(dv_s)

    dq_s[...] = jnp.zeros_like(dq_s)
    lses = [lse_ref[i : i + 1, :] * LOG2E for i in range(heads)]

    def block(j, masked):
        here = pl.ds(j * size, size)
        scores = [_dot_t(k_ref[i, here, :], q_ref[i]) for i in range(heads)]
        dps = [_dot_t(v_ref[i, here, :], do_ref[i]) for i in range(heads)]
        ok = _iota(size, 1) >= _iota(size, 0)
        for i in range(heads):
            p = jnp.exp2(scores[i] * e - lses[i])
            if masked:
                p = jnp.where(ok, p, 0.0)
            ds = (p * (dps[i] - delta_ref[i : i + 1, :])).astype(bf16)
            dv_s[i, here, :] += _dot(p.astype(bf16), do_ref[i])
            dk_s[i, here, :] += _dot(ds, q_ref[i])
            dq_s[i] += _dot(k_ref[i, here, :].T, ds)

    _strips(iq, k_ref.shape[1] // size, block)
    for i in range(heads):
        dq_ref[i] = (dq_s[i] * scale).T.astype(bf16)

    @pl.when(iq == pl.num_programs(0) - 1)
    def _():
        dk_ref[...] = (dk_s[...] * scale).astype(bf16)
        dv_ref[...] = dv_s[...].astype(bf16)


def attend_back(q, k, v, do, lse, delta):
    heads, t, d = q.shape
    size = QUERIES
    block = pl.BlockSpec((heads, size, d), lambda i: (0, i, 0))
    whole = pl.BlockSpec((heads, t, d), lambda i: (0, 0, 0))
    row = pl.BlockSpec((heads, size), lambda i: (0, i))
    return pl.pallas_call(
        functools.partial(_attend_back, scale=d**-0.5),
        grid=(t // size,),
        in_specs=[block, whole, whole, block, row, row],
        out_specs=[block, whole, whole],
        out_shape=[jax.ShapeDtypeStruct(q.shape, bf16)] * 3,
        scratch_shapes=[pltpu.VMEM((heads, d, size), f32), pltpu.VMEM((heads, t, d), f32), pltpu.VMEM((heads, t, d), f32)],
        compiler_params=PARAMS,
        cost_estimate=_cost(5 * heads * t * t * d, q, q, q, q, q, q),
        name="attend_back",
    )(q, k, v, do, lse, delta)


def _scaled(h):
    h = h.astype(f32)
    r = lax.rsqrt(jnp.mean(h * h, -1, keepdims=True) + EPS)
    return h, r, (h * r).astype(bf16)


def _scaled_back(h, r, db):
    return r * db - h * (r * r * r * jnp.mean(db * h, -1, keepdims=True))


def _angles(coarse_ref, fine_ref):
    ca, sa = (coarse_ref[i][:, None, :] for i in BOTH)
    cb, sb = (fine_ref[i][None] for i in BOTH)
    shape = (ca.shape[0] * cb.shape[1], ca.shape[2])
    return (ca * cb - sa * sb).reshape(shape), (sa * cb + ca * sb).reshape(shape)


def angle_tables(tokens):
    half = HEAD // 2
    slow = THETA ** (-np.arange(half) / half)
    tables = ((np.arange(0, tokens, FINE), (np.arange(FINE))))
    return [jnp.asarray(np.stack([np.cos(p[:, None] * slow), np.sin(p[:, None] * slow)]), f32) for p in tables]


def _turned(t, cos, sin):
    half = t.shape[1] // 2
    a, b = t[:, :half].astype(f32), t[:, half:].astype(f32)
    return jnp.concatenate([a * cos - b * sin, b * cos + a * sin], 1).astype(bf16)


def _qkv(h_ref, w_ref, coarse_ref, fine_ref, *outs):
    cos, sin = _angles(coarse_ref, fine_ref)
    heads, _, d = outs[0].shape
    _, _, a = _scaled(h_ref[...])
    t = _dot(a, w_ref[...]).astype(bf16)
    for n, out in enumerate(outs):
        for i in range(heads):
            at = (n * heads + i) * d
            one = t[:, at : at + d]
            out[i] = one if n == 2 else _turned(one, cos, sin)


def _qkv_back(h_ref, dq_ref, dk_ref, dv_ref, coarse_ref, fine_ref, w_ref, dmid_ref, *rest, inner):
    dh_ref, (dw_ref, acc) = (rest[0], rest[1:]) if inner else (None, rest)
    heads = dq_ref.shape[0]
    step = pl.program_id(0)
    _cleared(acc)
    h, r, a = _scaled(h_ref[...])
    cos, sin = _angles(coarse_ref, fine_ref)
    back = [_turned(ref[i], cos, -sin) for ref in (dq_ref, dk_ref) for i in range(heads)]
    d = jnp.concatenate(back + [dv_ref[i] for i in range(heads)], 1)
    acc[...] += _dot(a.T, d)
    if inner:
        da = _dot_t(d, w_ref[...]).astype(bf16).astype(f32)
        dh_ref[...] = (dmid_ref[...].astype(f32) + _scaled_back(h, r, da)).astype(bf16)

    @pl.when(step == pl.num_programs(0) - 1)
    def _():
        dw_ref[...] = acc[...].astype(bf16)


def _cleared(*sums):
    @pl.when(pl.program_id(0) == 0)
    def _():
        for ref in sums:
            ref[...] = jnp.zeros(ref.shape, f32)


def _middle(h, o_ref, wo_ref):
    d = o_ref.shape[2]
    got = sum(_dot(o_ref[i], wo_ref[i * d : (i + 1) * d, :]) for i in range(o_ref.shape[0]))
    return (h.astype(f32) + got.astype(bf16).astype(f32)).astype(bf16)


def _silu(gate):
    s = jax.nn.sigmoid(gate)
    return s, gate * s


def _hidden(h_ref, o_ref, wo_ref, wg_ref, wu_ref, wd_ref, mid_ref, next_ref):
    mid = _middle(h_ref[...], o_ref, wo_ref)
    mid_ref[...] = mid
    h, _, b = _scaled(mid)

    def one(c, total):
        cols = pl.ds(c * CHUNK, CHUNK)
        _, silu = _silu(_dot(b, wg_ref[:, cols]))
        act = (silu * _dot(b, wu_ref[:, cols])).astype(bf16)
        return total + _dot(act, wd_ref[cols, :])

    out = lax.fori_loop(0, wg_ref.shape[1] // CHUNK, one, jnp.zeros(h.shape, f32), unroll=True)
    next_ref[...] = (h + out.astype(bf16).astype(f32)).astype(bf16)


def _hidden_back(h_ref, o_ref, dy_ref, wo_ref, wg_ref, wu_ref, wd_ref, dmid_ref, do_ref, delta_ref, dwo_ref, dwg_ref, dwu_ref, dwd_ref,
                 mid_s, b_s, bt_s, dyt_s, db_s, act_s, dgate_s, dup_s, *, last):
    step = pl.program_id(0)
    heads, t, d = o_ref.shape
    tiles = t // TILE

    @pl.when(step == 0)
    def _():
        def one(i, _):
            rows = pl.ds(i * TILE, TILE)
            mid = _middle(h_ref[rows, :], o_ref.at[:, rows, :], wo_ref) if last else h_ref[rows, :]
            mid_s[rows, :] = mid
            b = _scaled(mid)[2]
            b_s[rows, :] = b
            bt_s[:, rows] = b.T
            dyt_s[:, rows] = dy_ref[rows, :].T
            db_s[rows, :] = jnp.zeros((TILE, db_s.shape[1]), f32)

        _loop(tiles, one)

    def part(i, _):
        rows = pl.ds(i * SUB, SUB)
        b = b_s[rows, :]
        s, silu = _silu(_dot(b, wg_ref[...]))
        up = _dot(b, wu_ref[...])
        dact = _dot_t(dy_ref[rows, :], wd_ref[...]).astype(bf16).astype(f32)
        dup = (dact * silu).astype(bf16)
        dgate = (dact * up * (s + silu - silu * s)).astype(bf16)
        act_s[rows, :] = (silu * up).astype(bf16)
        dgate_s[rows, :] = dgate
        dup_s[rows, :] = dup
        db_s[rows, :] += _dot_t(dgate, wg_ref[...]) + _dot_t(dup, wu_ref[...])

    for i in range(t // SUB):
        part(i, None)
    dwd_ref[...] = _dot(dyt_s[...], act_s[...]).T.astype(bf16)
    dwg_ref[...] = _dot(bt_s[...], dgate_s[...]).astype(bf16)
    dwu_ref[...] = _dot(bt_s[...], dup_s[...]).astype(bf16)

    @pl.when(step == pl.num_programs(0) - 1)
    def _():
        def one(i, _):
            rows = pl.ds(i * TILE, TILE)
            h, r, _ = _scaled(mid_s[rows, :])
            db = db_s[rows, :].astype(bf16).astype(f32)
            dmid = (dy_ref[rows, :].astype(f32) + _scaled_back(h, r, db)).astype(bf16)
            dmid_ref[rows, :] = dmid
            do = _dot_t(dmid, wo_ref[...]).astype(bf16)
            for n in range(heads):
                mine, o = do[:, n * d : (n + 1) * d], o_ref[n, rows, :]
                do_ref[n, rows, :] = mine
                delta_ref[n : n + 1, rows] = jnp.sum((mine.astype(f32) * o.astype(f32)).T, axis=0, keepdims=True)
                bt_s[n * d : (n + 1) * d, rows] = o.T

        _loop(tiles, one)
        dwo_ref[...] = _dot(bt_s[...], dmid_ref[...]).astype(bf16)


class Layer:
    def __init__(self, packed, down, tokens, tables):
        self.packed, self.down = packed, down
        d, f = down.shape[1], down.shape[0]
        self.d, self.f, self.heads, self.t = d, f, d // HEAD, tokens
        part = lambda size, at: pl.BlockSpec((d, size), lambda i: (0, at // size), pipeline_mode=ONCE)
        self.w_qkv = part(3 * d, 0)
        self.w_hidden = [part(d, 3 * d), part(f, 4 * d), part(f, 4 * d + f), pl.BlockSpec((f, d), lambda i: (0, 0), pipeline_mode=ONCE)]
        self.rows = pl.BlockSpec((TILE, d), lambda i: (i, 0))
        angle = lambda table, rows, at: pl.BlockSpec((2, rows, table.shape[2]), lambda i: (0, at * i, 0))
        self.angles = [(tables[0], angle(tables[0], TILE // FINE, 1)), (tables[1], angle(tables[1], FINE, 0))]
        self.split = pl.BlockSpec((self.heads, TILE, HEAD), lambda i: (0, i, 0))
        self.row = pl.BlockSpec((self.heads, TILE), lambda i: (0, i))
        self.states = jax.ShapeDtypeStruct((self.t, d), bf16)
        self.parts = jax.ShapeDtypeStruct((self.heads, self.t, HEAD), bf16)

    def call(self, body, name, flops, ins, outs, scratch=()):
        arrays = [a for a, _ in ins]
        return pl.pallas_call(
            body, grid=(self.t // TILE,), in_specs=[s for _, s in ins], out_specs=[s for _, s in outs], out_shape=[a for a, _ in outs],
            scratch_shapes=[pltpu.VMEM(s, f32) for s in scratch], compiler_params=PARAMS,
            cost_estimate=_cost(2 * self.t * flops, *arrays), name=name)(*arrays)

    def whole(self, *shape):
        return jax.ShapeDtypeStruct(shape, bf16), pl.BlockSpec(shape, lambda i: (0, 0), pipeline_mode=ONCE)

    def hidden_weights(self):
        return list(zip((self.packed, self.packed, self.packed, self.down), self.w_hidden))

    def qkv(self, h):
        ins = [(h, self.rows), (self.packed, self.w_qkv), *self.angles]
        return self.call(_qkv, "qkv", 3 * self.d * self.d, ins, [(self.parts, self.split)] * 3)

    def hidden(self, h, o):
        flops = self.d * self.d + 3 * self.d * self.f
        return self.call(_hidden, "hidden", flops, [(h, self.rows), (o, self.split), *self.hidden_weights()], [(self.states, self.rows)] * 2)

    def hidden_back(self, h, o, dy, last):
        d, f, t, size = self.d, self.f, self.t, HCHUNK
        full = lambda *shape: pl.BlockSpec(shape, lambda c: (0,) * len(shape), pipeline_mode=ONCE)
        columns = lambda at: pl.BlockSpec((d, size), lambda c: (0, at // size + c))
        ins = [full(t, d), full(*o.shape), full(t, d), self.w_hidden[0], columns(4 * d), columns(4 * d + f), pl.BlockSpec((size, d), lambda c: (c, 0))]
        slim = pl.BlockSpec((d, size), lambda c: (0, c))
        outs = [full(t, d), full(*o.shape), full(self.heads, t), full(d, d), slim, slim, pl.BlockSpec((size, d), lambda c: (c, 0))]
        shape = lambda *s: jax.ShapeDtypeStruct(s, bf16)
        given = [h, o, dy, self.packed, self.packed, self.packed, self.down]
        vmem = lambda *s: pltpu.VMEM(s, bf16)
        return pl.pallas_call(
            functools.partial(_hidden_back, last=last), grid=(f // size,), in_specs=ins, out_specs=outs,
            out_shape=[self.states, self.parts, jax.ShapeDtypeStruct((self.heads, t), f32), shape(d, d), shape(d, f), shape(d, f), shape(f, d)],
            scratch_shapes=[vmem(t, d), vmem(t, d), vmem(d, t), vmem(d, t), pltpu.VMEM((t, d), f32), vmem(t, size), vmem(t, size), vmem(t, size)],
            compiler_params=PARAMS, cost_estimate=_cost(t * d * f * 16, *given), name="hidden_back")(*given)

    def qkv_back(self, h, dqkv, dmid, inner):
        d = self.d
        ins = [(h, self.rows)] + [(a, self.split) for a in dqkv] + [*self.angles, (self.packed, self.w_qkv), (dmid, self.rows)]
        outs = ([(self.states, self.rows)] if inner else []) + [self.whole(d, 3 * d)]
        return self.call(functools.partial(_qkv_back, inner=inner), "qkv_back", 6 * d * d, ins, outs, [(d, 3 * d)])


def _update(squares_ref, *refs, count):
    (gp_ref, gd_ref), (w, m, v), (new_w, new_m, new_v) = refs[:2], (refs[i : i + 7] for i in (2, 9, 16)), (refs[i : i + 7] for i in (23, 30, 37))
    factor = jnp.minimum(1.0, 0.5 * lax.rsqrt(jnp.sum(squares_ref[...], keepdims=True) / count + 1e-30))
    at = 0
    for i in range(7):
        cols = w[i].shape[2]

        def one(layer, _):
            g = gd_ref[layer] if i == 6 else gp_ref[layer, :, at : at + cols]
            g = g.astype(f32) * factor
            mm = 0.9 * m[i][layer] + 0.1 * g
            vv = 0.95 * v[i][layer] + 0.05 * g * g
            new_m[i][layer] = mm
            new_v[i][layer] = vv
            old = w[i][layer].astype(f32)
            new_w[i][layer] = (old - 0.02 * (mm * lax.rsqrt(vv + 1e-8) + 0.1 * old)).astype(bf16)

        _loop(w[i].shape[0], one)
        at += cols


def updated(squares, gp, gd, weights, m, v, count):
    given = [squares, gp, gd, *weights, *m, *v]
    spec = pl.BlockSpec(memory_space=pltpu.VMEM)
    return pl.pallas_call(
        functools.partial(_update, count=count),
        in_specs=[spec] * len(given),
        out_specs=[spec] * 21,
        out_shape=[jax.ShapeDtypeStruct(a.shape, a.dtype) for a in (*weights, *m, *v)],
        compiler_params=pltpu.CompilerParams(vmem_limit_bytes=VMEM),
        cost_estimate=_cost(gp.size, *given),
        name="update",
    )(*given)


MESH = pl.DeviceIdType.MESH


class Place:
    def __init__(self, n):
        self.n, self.side = n, math.isqrt(n // 2)
        self.me = lax.axis_index("dp")
        self.core = lax.rem(self.me, 2)
        chip = lax.div(self.me, 2)
        self.at = (lax.div(chip, self.side), lax.rem(chip, self.side))

    def index(self, x, y, core):
        return (x * self.side + y) * 2 + core

    def moved(self, axis, by):
        at = list(self.at)
        at[axis] = lax.rem(at[axis] + (by + self.side), self.side)
        return self.index(*at, self.core)

    def partner(self):
        return self.index(*self.at, 1 - self.core)

    def off(self, axis, by):
        return lax.rem(self.at[axis] + (by + self.side), self.side)


def _send(src, dst, send, recv, to):
    copy = pltpu.make_async_remote_copy(src_ref=src, dst_ref=dst, send_sem=send, recv_sem=recv, device_id={"dp": to}, device_id_type=MESH)
    copy.start()
    return copy


def _gather(n, p_in, d_in, *rest):
    outs, (send, recv, pair_send, pair_recv, own_sem) = (rest[:2], rest[2:4]), rest[4:]
    me = Place(n)
    partner = me.partner()
    barrier = pltpu.get_barrier_semaphore()
    near = [me.moved(0, 1), me.moved(0, -1), me.moved(1, 1), me.moved(1, -1), partner]
    for to in near:
        pl.semaphore_signal(barrier, inc=1, device_id={"dp": to}, device_id_type=MESH)
    pl.semaphore_wait(barrier, len(near))

    wide = p_in.shape[2] // 2
    tall = d_in.shape[1] // 2
    sent = []

    def block(which, layer, i, j, core, half=None):
        x, y = (i, j) if layer == 0 else (j, i)
        ref = outs[layer][which].at[x, y, core]
        if half is None:
            return ref
        return ref.at[:, pl.ds(half * wide, wide)] if which == 0 else ref.at[pl.ds(half * tall, tall), :]

    places = (0, -1, 1, 2)
    order = lambda layer: (layer, 1 - layer)

    def whole(layer, walk, source=None):
        first, second = order(layer)
        i = me.off(first, 0 if walk == 0 else places[walk - 1])
        axis = first if walk == 0 else second
        for d, by in WAYS:
            for which in BOTH:
                dst = block(which, layer, i, me.at[second], me.core)
                sent.append(_send(dst if source is None else source[which].at[layer], dst, send.at[layer, walk, d, which], recv.at[layer, walk, d, which],
                                  me.moved(axis, by)))

    def there(layer, walk, by):
        first, second = order(layer)
        if walk == 0:
            return me.off(first, by), me.at[second]
        return me.off(first, places[walk - 1]), me.off(second, by)

    def forward(layer, walk):
        first, second = order(layer)
        axis = first if walk == 0 else second
        for d, by in WAYS:
            i, j = there(layer, walk, -by)
            for which in BOTH:
                got = block(which, layer, i, j, me.core)
                pltpu.make_async_remote_copy(src_ref=got, dst_ref=got, send_sem=send.at[layer, walk, d, which], recv_sem=recv.at[layer, walk, d, which],
                                             device_id={"dp": me.moved(axis, -by)}, device_id_type=MESH).wait_recv()
                part = block(which, layer, i, j, me.core, d)
                sent.append(_send(part, part, send.at[layer, walk, 2 + d, which], recv.at[layer, walk, 2 + d, which], me.moved(axis, by)))
            share(layer, i, j)

    def finish(layer, walk):
        first, second = order(layer)
        axis = first if walk == 0 else second
        i, j = there(layer, walk, 2)
        for d, by in WAYS:
            for which in BOTH:
                part = block(which, layer, i, j, me.core, d)
                pltpu.make_async_remote_copy(src_ref=part, dst_ref=part, send_sem=send.at[layer, walk, 2 + d, which], recv_sem=recv.at[layer, walk, 2 + d, which],
                                             device_id={"dp": me.moved(axis, -by)}, device_id_type=MESH).wait_recv()
        share(layer, i, j)

    count = [0, 0]
    shared = [[], []]

    def share(layer, i, j, source=None):
        for which in BOTH:
            dst = block(which, layer, i, j, me.core)
            k = count[layer]
            sent.append(_send(dst if source is None else source[which].at[layer], dst, pair_send.at[layer, k, which], pair_recv.at[layer, k, which], partner))
        shared[layer].append((i, j))
        count[layer] += 1

    given = (p_in, d_in)
    own = []
    for layer in BOTH:
        whole(layer, 0, given)
    for layer in BOTH:
        whole(layer, 1, given)
    for layer in BOTH:
        first, second = order(layer)
        share(layer, me.at[first], me.at[second], given)
        for which in BOTH:
            copy = pltpu.make_async_copy(given[which].at[layer], block(which, layer, me.at[first], me.at[second], me.core), own_sem.at[layer, which])
            copy.start()
            own.append(copy)
    for layer in BOTH:
        forward(layer, 0)
        whole(layer, 2)
        whole(layer, 3)
    for layer in BOTH:
        forward(layer, 1)
    for layer in BOTH:
        finish(layer, 0)
        whole(layer, 4)
    for walk in (2, 3):
        for layer in BOTH:
            forward(layer, walk)
    for layer in BOTH:
        finish(layer, 1)
    for layer in BOTH:
        forward(layer, 4)
    for walk in (2, 3, 4):
        for layer in BOTH:
            finish(layer, walk)
    for copy in own:
        copy.wait()
    for layer in BOTH:
        for k, (i, j) in enumerate(shared[layer]):
            for which in BOTH:
                got = block(which, layer, i, j, 1 - me.core)
                pltpu.make_async_remote_copy(src_ref=got, dst_ref=got, send_sem=pair_send.at[layer, k, which], recv_sem=pair_recv.at[layer, k, which],
                                             device_id={"dp": partner}, device_id_type=MESH).wait_recv()
    for copy in sent:
        copy.wait_send()


def gathered(n, weights):
    packed = jnp.concatenate(weights[:6], axis=2)
    down = weights[6]
    side = math.isqrt(n // 2)
    layers, r, wide = packed.shape
    rd, cd = down.shape[1:]
    dma = pltpu.SemaphoreType.DMA
    whole = pl.pallas_call(
        functools.partial(_gather, n),
        out_shape=[jax.ShapeDtypeStruct((side, side, 2, *s), bf16) for s in ((r, wide), (rd, cd))] * layers,
        in_specs=[pl.BlockSpec(memory_space=pltpu.VMEM)] * 2,
        out_specs=[pl.BlockSpec(memory_space=pl.ANY)] * (2 * layers),
        scratch_shapes=[dma((layers, 5, 4, 2)), dma((layers, 5, 4, 2)), dma((layers, side * side, 2)), dma((layers, side * side, 2)), dma((layers, 2))],
        compiler_params=pltpu.CompilerParams(collective_id=1, has_side_effects=True),
        name="gather",
    )(packed, down)
    return [[a.reshape(-1, a.shape[-1]) for a in whole[at : at + 2]] for at in range(0, 2 * layers, 2)]


def _reduce(n, *refs):
    grads, rest = (refs[:5], refs[5:10]), refs[10:]
    p_out, d_out, sq_out = rest[:3]
    (own_p, own_d, two_p, two_d, far_p, far_d, near_p, near_d, bfar_p, bfar_d, bnear_p, bnear_d, sq,
     load, pair_send, pair_recv, a_send, a_recv, b_send, b_recv, sq_send, sq_recv) = rest[3:]
    me = Place(n)
    partner, core, side = me.partner(), me.core, me.side
    barrier = pltpu.get_barrier_semaphore()

    def greet(k, _):
        pl.semaphore_signal(barrier, inc=1, device_id={"dp": lax.rem(me.me + k, n)}, device_id_type=MESH)

    lax.fori_loop(1, n, greet, None)
    pl.semaphore_wait(barrier, n - 1)

    own, two = (own_p, own_d), (two_p, two_d)
    order = lambda layer: (layer, 1 - layer)
    places = (2, 1, -1, 0)
    sent = []

    def chunk(layer, k):
        return me.off(order(layer)[0], places[k])

    for k in range(side):
        for layer in BOTH:
            i = chunk(layer, k)
            at = 0
            for w in range(5):
                g = grads[layer][w]
                mine, theirs = ((g.at[i, :, c] if layer == 0 else g.at[:, i, c]) for c in (core, 1 - core))
                which = 0 if w < 4 else 1
                cols = g.shape[4]
                window = lambda buf: buf.at[layer, i, :, :, pl.ds(at, cols)] if which == 0 else buf.at[layer, i]
                pltpu.make_async_copy(mine, window(own[which]), load.at[layer, k, which]).start()
                sent.append(_send(theirs, window(two[which]), pair_send.at[layer, k, which, w], pair_recv.at[layer, k, which], partner))
                at += cols

    def have(layer, k):
        i = chunk(layer, k)
        for which in BOTH:
            pltpu.make_async_copy(own[which].at[layer, i], own[which].at[layer, i], load.at[layer, k, which]).wait()
            got = two[which].at[layer, i]
            pltpu.make_async_remote_copy(src_ref=got, dst_ref=got, send_sem=pair_send.at[layer, k, which, 0], recv_sem=pair_recv.at[layer, k, which],
                                         device_id={"dp": partner}, device_id_type=MESH).wait_recv()

    wide, tall = own_p.shape[4] // 2, own_d.shape[3] // 2
    piece = wide // 2

    def over(which, half, body):
        if which == 1:
            part = slice(None) if half is None else slice(half * tall, half * tall + tall)
            body((part, slice(None)), (slice(None), slice(None)))
        else:
            first = 0 if half is None else 2 * half
            columns = lambda k: (slice(None), pl.ds(pl.multiple_of(k * piece, 128), piece))
            _loop(4 if half is None else 2, lambda k, _: body(columns(first + k), columns(k)))

    def both(layer, i, lo, hi):
        def one(j, _):
            for which in BOTH:
                def body(at, _):
                    own[which][(layer, i, j) + at] = (own[which][(layer, i, j) + at].astype(f32) + two[which][(layer, i, j) + at].astype(f32)).astype(bf16)
                over(which, None, body)
        lax.fori_loop(lo, hi, one, None)

    h = side // 2

    def a_part(which, layer, i, half):
        return own[which].at[layer, i, pl.ds(half * h, h)]

    def a_send_one(layer, d, stage, src, dst):
        by = STEP[d]
        for which in BOTH:
            sent.append(_send(src[which], dst[which], a_send.at[layer, d, stage, which], a_recv.at[layer, d, stage, which], me.moved(order(layer)[0], by)))

    def a_wait(layer, d, stage, dst):
        by = STEP[d]
        for which in BOTH:
            pltpu.make_async_remote_copy(src_ref=dst[which], dst_ref=dst[which], send_sem=a_send.at[layer, d, stage, which], recv_sem=a_recv.at[layer, d, stage, which],
                                         device_id={"dp": me.moved(order(layer)[0], -by)}, device_id_type=MESH).wait_recv()

    far, near = (far_p, far_d), (near_p, near_d)
    far_at = lambda layer, d: [ref.at[layer, d] for ref in far]
    near_at = lambda layer, d, half: [ref.at[layer, d, pl.ds(half * h, h)] for ref in near]
    for layer in BOTH:
        have(layer, 0)
        i = chunk(layer, 0)
        both(layer, i, 0, side)
        for d in BOTH:
            a_send_one(layer, d, 0, [a_part(w, layer, i, d) for w in BOTH], far_at(layer, d))
    for layer in BOTH:
        for d in BOTH:
            have(layer, 1 + d)
            i = chunk(layer, 1 + d)
            both(layer, i, (1 - d) * h, (1 - d) * h + h)
            a_send_one(layer, d, 1, [a_part(w, layer, i, 1 - d) for w in BOTH], near_at(layer, d, 1 - d))
    for layer in BOTH:
        for d in BOTH:
            i = chunk(layer, 1 + d)
            a_wait(layer, d, 0, far_at(layer, d))

            def one(j, _):
                b = d * h + j
                for which in BOTH:
                    def body(at, _):
                        own[which][(layer, i, b) + at] = (own[which][(layer, i, b) + at].astype(f32) + two[which][(layer, i, b) + at].astype(f32)
                                                          + far[which][(layer, d, j) + at].astype(f32)).astype(bf16)
                    over(which, None, body)

            _loop(h, one)
            a_send_one(layer, d, 2, [a_part(w, layer, i, d) for w in BOTH], near_at(layer, d, d))
    bfar, bnear = (bfar_p, bfar_d), (bnear_p, bnear_d)
    def half_of(which, ref, half):
        return ref.at[:, pl.ds(half * wide, wide)] if which == 0 else ref.at[pl.ds(half * tall, tall), :]

    def b_send_one(layer, d, stage, src, dst):
        by = STEP[d]
        for which in BOTH:
            sent.append(_send(src[which], dst[which], b_send.at[layer, d, stage, which], b_recv.at[layer, d, stage, which], me.moved(order(layer)[1], by)))

    def b_wait(layer, d, stage, dst):
        by = STEP[d]
        for which in BOTH:
            pltpu.make_async_remote_copy(src_ref=dst[which], dst_ref=dst[which], send_sem=b_send.at[layer, d, stage, which], recv_sem=b_recv.at[layer, d, stage, which],
                                         device_id={"dp": me.moved(order(layer)[1], -by)}, device_id_type=MESH).wait_recv()

    def four(which, layer, i, j, cut):
        return (own[which][(layer, i, j) + cut].astype(f32) + two[which][(layer, i, j) + cut].astype(f32)
                + near[which][(layer, 0, j) + cut].astype(f32) + near[which][(layer, 1, j) + cut].astype(f32))

    bfar_at = lambda layer, d: [ref.at[layer, d] for ref in bfar]
    bnear_at = lambda layer, d, half: [half_of(w, bnear[w].at[layer, d], half) for w in BOTH]
    for layer in BOTH:
        have(layer, 3)
        for d in BOTH:
            a_wait(layer, d, 1, near_at(layer, d, 1 - d))
            a_wait(layer, d, 2, near_at(layer, d, d))
        second = order(layer)[1]
        i = chunk(layer, 3)
        for j, kept in ((me.off(second, 2), None), (me.off(second, 1), 0), (me.off(second, -1), 1)):
            for which in BOTH:
                def body(at, _):
                    own[which][(layer, i, j) + at] = four(which, layer, i, j, at).astype(bf16)
                over(which, None if kept is None else 1 - kept, body)
        for d in BOTH:
            j = me.off(second, 2)
            b_send_one(layer, d, 0, [half_of(w, own[w].at[layer, i, j], d) for w in BOTH], bfar_at(layer, d))
        for d in BOTH:
            j = me.off(second, STEP[d])
            b_send_one(layer, d, 1, [half_of(w, own[w].at[layer, i, j], 1 - d) for w in BOTH], bnear_at(layer, d, 1 - d))
    for layer in BOTH:
        second = order(layer)[1]
        i = chunk(layer, 3)
        for d in BOTH:
            j = me.off(second, STEP[d])
            b_wait(layer, d, 0, bfar_at(layer, d))
            for which in BOTH:
                def body(at, here):
                    bfar[which][(layer, d) + here] = (four(which, layer, i, j, at) + bfar[which][(layer, d) + here].astype(f32)).astype(bf16)
                over(which, d, body)
            b_send_one(layer, d, 2, bfar_at(layer, d), bnear_at(layer, d, d))
    sq[me.me] = jnp.zeros(sq.shape[1:], f32)
    for layer in BOTH:
        second = order(layer)[1]
        i, j = chunk(layer, 3), me.at[second]
        for d in BOTH:
            b_wait(layer, d, 1, bnear_at(layer, d, 1 - d))
            b_wait(layer, d, 2, bnear_at(layer, d, d))
        for which, out in ((0, p_out), (1, d_out)):
            def body(at, _):
                g = (four(which, layer, i, j, at) + bnear[which][(layer, 0) + at].astype(f32) + bnear[which][(layer, 1) + at].astype(f32)).astype(bf16)
                out[(layer,) + at] = g
                g = g.astype(f32)
                g = g * g
                rows, cols = g.shape
                sq[me.me] += sum(g[a : a + 8, b : b + 128] for a in range(0, rows, 8) for b in range(0, cols, 128))
            over(which, None, body)
    def tell(k, _):
        to = lax.rem(me.me + k, n)
        pltpu.make_async_remote_copy(src_ref=sq.at[me.me], dst_ref=sq.at[me.me], send_sem=sq_send.at[k], recv_sem=sq_recv.at[n - k],
                                     device_id={"dp": to}, device_id_type=MESH).start()

    def hear(k, _):
        who = lax.rem(me.me + k, n)
        pltpu.make_async_remote_copy(src_ref=sq.at[who], dst_ref=sq.at[who], send_sem=sq_send.at[k], recv_sem=sq_recv.at[k],
                                     device_id={"dp": who}, device_id_type=MESH).wait_recv()

    def told(k, _):
        to = lax.rem(me.me + k, n)
        pltpu.make_async_remote_copy(src_ref=sq.at[me.me], dst_ref=sq.at[me.me], send_sem=sq_send.at[k], recv_sem=sq_recv.at[n - k],
                                     device_id={"dp": to}, device_id_type=MESH).wait_send()

    lax.fori_loop(1, n, tell, None)
    lax.fori_loop(1, n, hear, None)
    sq_out[...] = jnp.sum(sq[...], axis=0)
    lax.fori_loop(1, n, told, None)
    for copy in sent:
        copy.wait_send()


def reduced(n, grads):
    side = math.isqrt(n // 2)
    layers = len(grads)
    r, rd = grads[0][0].shape[0] // n, grads[0][-1].shape[0] // n
    cd = grads[0][-1].shape[1]
    wide = sum(g.shape[1] for g in grads[0][:-1])
    dma, vmem = pltpu.SemaphoreType.DMA, pltpu.VMEM
    h = side // 2
    cut = [g.reshape(side, side, 2, g.shape[0] // n, g.shape[1]) for layer in grads for g in layer]
    return pl.pallas_call(
        functools.partial(_reduce, n),
        out_shape=[jax.ShapeDtypeStruct((layers, r, wide), bf16), jax.ShapeDtypeStruct((layers, rd, cd), bf16), jax.ShapeDtypeStruct((8, 128), f32)],
        in_specs=[pl.BlockSpec(memory_space=pl.ANY)] * len(cut),
        out_specs=[pl.BlockSpec(memory_space=pltpu.VMEM)] * 3,
        scratch_shapes=[
            vmem((layers, side, side, r, wide), bf16), vmem((layers, side, side, rd, cd), bf16),
            vmem((layers, side, side, r, wide), bf16), vmem((layers, side, side, rd, cd), bf16),
            vmem((layers, 2, h, r, wide), bf16), vmem((layers, 2, h, rd, cd), bf16),
            vmem((layers, 2, side, r, wide), bf16), vmem((layers, 2, side, rd, cd), bf16),
            vmem((layers, 2, r, wide // 2), bf16), vmem((layers, 2, rd // 2, cd), bf16),
            vmem((layers, 2, r, wide), bf16), vmem((layers, 2, rd, cd), bf16),
            vmem((n, 8, 128), f32),
            dma((layers, side, 2)), dma((layers, side, 2, 5)), dma((layers, side, 2)),
            dma((layers, 2, 3, 2)), dma((layers, 2, 3, 2)), dma((layers, 2, 3, 2)), dma((layers, 2, 3, 2)),
            dma((n,)), dma((n,)),
        ],
        compiler_params=pltpu.CompilerParams(collective_id=2, has_side_effects=True, vmem_limit_bytes=48 * 2**20),
        name="reduce",
    )(*cut)


def solution(mesh):
    n = mesh.shape["dp"]

    def step(x, dy, *arrays):
        weights, m, v = (arrays[i : i + 7] for i in (0, 7, 14))
        whole = gathered(n, weights)
        tables = angle_tables(x.shape[1])
        first, second = (Layer(*w, x.shape[1], tables) for w in whole)
        x = x[0]
        qkv0 = first.qkv(x)
        o0, lse0 = attend(*qkv0)
        mid0, h = first.hidden(x, o0)
        qkv1 = second.qkv(h)
        o1, lse1 = attend(*qkv1)
        dmid, do, delta, *by_hidden1 = second.hidden_back(h, o1, dy[0], True)
        dh, by_qkv1 = second.qkv_back(h, attend_back(*qkv1, do, lse1, delta), dmid, True)
        dmid, do, delta, *by_hidden0 = first.hidden_back(mid0, o0, dh, False)
        (by_qkv0,) = first.qkv_back(x, attend_back(*qkv0, do, lse0, delta), dmid, False)
        gp, gd, squares = reduced(n, [[by_qkv0, *by_hidden0], [by_qkv1, *by_hidden1]])
        return tuple(updated(squares, gp, gd, weights, m, v, n * (gp.size + gd.size)))

    states, cut = P(("rep", "dp"), None, None), P(None, "dp", None)
    return jax.shard_map(
        step,
        mesh=mesh,
        in_specs=(states, states) + (cut,) * 21,
        out_specs=(P("rep", "dp", None),) * 21,
        check_vma=False,
    )
```
